32 devices in a mesh: grp: 16 (over z, y, x), box: 2 (over core).
Axes of the slice: x: 2, y: 2, z: 4, core: 2. Of those that a mesh axis runs over, the one named last changes fastest.
Arguments:
- fine_state: float32 [16, 5, 8, 16, 256], P('grp', None, 'box'), may hold values from -1 to 6, as said below
- patch_ghosts: float32 [16, 2, 2, 5, 16, 256], P('grp'), may hold values from -1 to 6, as said below
- coarse_state: float32 [16, 2, 24, 5, 128], P('grp', 'box'), may hold values from -1 to 6, as said below
- coarse_face_term: float32 [16, 2, 24, 5, 128], P('grp', 'box'), may hold values from -1 to 1
- dest_grp: int32 [16, 2, 24], P('grp', 'box'), may hold values from 0 to 15, as said below
- dest_column: int32 [16, 2, 24], P('grp', 'box'), may hold values from 0 to 23, as said below
Outputs:
- fine_new: float32 [16, 5, 8, 16, 256], P('grp', None, 'box')
- coarse_new: float32 [16, 2, 24, 5, 128], P('grp', 'box')
The draws below stay inside these ranges and needn't reach their ends.
Inputs may be any that keep to these rules, and one draw needn't show every extreme that they name: `fine_state`: every cell has density in 1 to 2, velocity components in -0.5 to 0.5 and pressure in 1 to 2. `patch_ghosts`: every cell has density in 1 to 2, velocity components in -0.5 to 0.5 and pressure in 1 to 2. `coarse_state`: every cell has density in 1 to 2, velocity components in -0.5 to 0.5 and pressure in 1 to 2. `dest_grp`: for each box index, each owner's columns receive exactly one record each; one box sends at most 2 and at least 1 records to each owner. `dest_column`: see dest_grp.
All inputs are finite; a program needn't handle non-finite values.
Results may differ from the reference program's by a relative error of at most 0.0001.
Values sent between devices are 32-bit elements; how exact they have to be, the bound alone decides.
No kernel may reach another device: no remote copies, remote signals or barrier semaphores. Data moves between devices by JAX's collectives and lax.ppermute only.
A program may use at most 64 MiB of HBM per device.

```python
import jax
import jax.numpy as jnp
from jax import lax

FIELDS = 5
FX = 4
FY = 16
FZ = 256
SUBSTEPS = 2
NXF = 8
CZ = 128
NCOL = 16
REC = 24
N_GRP = 16
N_BOX = 2


def conserved_draw(key, lead_shape, stack_axis):
    subkeys = jax.random.split(key, 5)
    uniforms = [jax.random.uniform(subkeys[member], lead_shape, jnp.float32) for member in range(5)]
    density = 1.0 + uniforms[0]
    velocity = [uniforms[member] - 0.5 for member in (1, 2, 3)]
    pressure = 1.0 + uniforms[4]
    kinetic = 0.5 * density * (velocity[0] ** 2 + velocity[1] ** 2 + velocity[2] ** 2)
    energy = pressure / 0.4 + kinetic
    members = [density, density * velocity[0], density * velocity[1], density * velocity[2], energy]
    return jnp.stack(members, axis=stack_axis)


def draw_fine_state(key, part):
    return conserved_draw(jax.random.fold_in(key, 11), (N_GRP, NXF, FY, FZ), 1)


def draw_patch_ghosts(key, part):
    return conserved_draw(jax.random.fold_in(key, 12), (N_GRP, 2, 2, FY, FZ), 3)


def draw_coarse_state(key, part):
    return conserved_draw(jax.random.fold_in(key, 13), (N_GRP, N_BOX, REC, CZ), 3)


def shuffle_columns(order_key):
    return jax.random.permutation(order_key, REC)


def routing(key):
    base = jax.random.fold_in(key, 7)
    plane_keys = jax.random.split(base, N_BOX)

    def plane(plane_key):
        first, second, third, fourth = jax.random.split(plane_key, 4)
        values = jnp.arange(N_GRP, dtype=jnp.int32)
        scores = jax.random.permutation(first, N_GRP).astype(jnp.int32)
        scores = jnp.where(values == 1, -2, jnp.where(values == N_GRP // 2, -1, scores))
        relabel = jnp.argsort(scores, stable=True).astype(jnp.int32)
        offsets = relabel[jnp.arange(REC) % N_GRP][jax.random.permutation(second, REC)]
        rotate = jax.random.randint(third, (N_GRP,), 0, REC)
        shifted = (jnp.arange(REC)[None, :] + rotate[:, None]) % REC
        owners = (jnp.arange(N_GRP)[:, None] + offsets[shifted]) % N_GRP
        orders = jax.vmap(shuffle_columns)(jax.random.split(fourth, N_GRP))
        columns = orders[owners, shifted]
        return (owners, columns)
    owners, columns = jax.vmap(plane)(plane_keys)
    return (owners.transpose(1, 0, 2).astype(jnp.int32), columns.transpose(1, 0, 2).astype(jnp.int32))


def draw_dest_grp(key, part):
    return routing(key)[0]


def draw_dest_column(key, part):
    return routing(key)[1]


def block_levels(own_key, dims, cuts, least, largest):
    factor_of, own = 1.0, jax.random.fold_in(own_key, 6)
    for axis_at, parts in cuts:
        draws = jnp.exp(jax.random.uniform(jax.random.fold_in(own, axis_at), (parts,), jnp.float32, least / len(cuts), largest / len(cuts)))
        factor_of = factor_of * jnp.repeat(draws, dims[axis_at] // parts).reshape([-1 if axis == axis_at else 1 for axis in range(len(dims))])
    return factor_of


def scatter_about(own_key, shape, scale, bound, cuts=(), kind=jnp.bfloat16):
    array = jax.random.normal(own_key, shape, jnp.float32) * scale
    if len(cuts) > 0:
        array = block_levels(own_key, shape, cuts, -0.22, 0.18) * array
    return jnp.clip(array, min=-bound, max=bound).astype(kind)


def setup_inputs(seed: int = 0) -> dict:
    arg_keys = jax.random.split(jax.random.key(seed), 7)
    return {
        "fine_state": draw_fine_state(jax.random.fold_in(arg_keys[6], 71), 0),
        "patch_ghosts": draw_patch_ghosts(jax.random.fold_in(arg_keys[6], 71), 0),
        "coarse_state": draw_coarse_state(jax.random.fold_in(arg_keys[6], 71), 0),
        "coarse_face_term": scatter_about(arg_keys[3], (N_GRP, N_BOX, REC, FIELDS, CZ), 0.2, 1.0, ((0, 16), (1, 2)), jnp.float32),
        "dest_grp": draw_dest_grp(jax.random.fold_in(arg_keys[6], 71), 0),
        "dest_column": draw_dest_column(jax.random.fold_in(arg_keys[6], 71), 0),
    }


gamma_ratio = 1.4
time_step = 0.06

def cell_values(conserved):
    density = conserved[0]
    velocity = conserved[1:4] / density
    kinetic = 0.5 * lax.optimization_barrier(jnp.sum(conserved[1:4] * velocity, axis=0))
    pressure = (gamma_ratio - 1.0) * (conserved[4] - kinetic)
    sound_speed = jnp.sqrt(gamma_ratio * pressure / density)
    return (velocity, pressure, sound_speed)

def physical_flux(conserved, velocity, pressure, normal):
    moving = velocity[normal]
    pieces = [conserved[1 + normal]]
    for member in range(3):
        if member == normal:
            pieces.append(conserved[1 + member] * moving + pressure)
        else:
            pieces.append(conserved[1 + member] * moving)
    pieces.append((conserved[4] + pressure) * moving)
    return jnp.stack(pieces)

def rusanov(left_state, right_state, left_flux, right_flux, left_speed, right_speed):
    biggest = jnp.maximum(left_speed, right_speed)
    return 0.5 * (left_flux + right_flux) - 0.5 * biggest * (right_state - left_state)

def advance(extended):
    velocity, pressure, sound_speed = cell_values(extended)
    cell_flux = physical_flux(extended, velocity, pressure, 0)
    cell_speed = jnp.abs(velocity[0]) + sound_speed
    face_flux = rusanov(extended[:, :-1], extended[:, 1:], cell_flux[:, :-1], cell_flux[:, 1:], cell_speed[:-1], cell_speed[1:])
    interior = extended[:, 1:-1]
    change = face_flux[:, 1:] - face_flux[:, :-1]
    inner_velocity = velocity[:, 1:-1]
    inner_pressure = pressure[1:-1]
    inner_sound = sound_speed[1:-1]
    for normal in (1, 2):
        side_flux = physical_flux(interior, inner_velocity, inner_pressure, normal)
        side_speed = jnp.abs(inner_velocity[normal]) + inner_sound
        grid_axis = normal + 1
        face_values = rusanov(interior, jnp.roll(interior, -1, grid_axis), side_flux, jnp.roll(side_flux, -1, grid_axis), side_speed, jnp.roll(side_speed, -1, normal))
        change = change + (face_values - jnp.roll(face_values, 1, grid_axis))
    return (interior - time_step * change, face_flux)

def patch_step(inputs):
    fine_patch, ghosts = inputs
    updated = fine_patch
    face_low = jnp.zeros((FIELDS, FY, FZ), jnp.float32)
    face_high = jnp.zeros((FIELDS, FY, FZ), jnp.float32)
    for substep in range(SUBSTEPS):
        time_frac = 0.5 * substep
        ghost_low = (1.0 - time_frac) * ghosts[0, 0] + time_frac * ghosts[1, 0]
        ghost_high = (1.0 - time_frac) * ghosts[0, 1] + time_frac * ghosts[1, 1]
        extended = jnp.concatenate([ghost_low[:, None], updated, ghost_high[:, None]], axis=1)
        updated, face_flux = advance(extended)
        face_low = face_low + face_flux[:, 0]
        face_high = face_high + face_flux[:, -1]
    return (updated, face_low, face_high)

def reference(fine_state, patch_ghosts, coarse_state, coarse_face_term, dest_grp, dest_column):
    fine_new, face_low, face_high = lax.map(patch_step, (fine_state, patch_ghosts))
    averaged = fine_new.reshape(N_GRP, FIELDS, NXF // 2, 2, FY // 2, 2, CZ, 2).mean(axis=(3, 5, 7))
    averaged = averaged.reshape(N_GRP, FIELDS, N_BOX, FX // 2, FY // 2, CZ)
    avg_records = averaged.transpose(0, 2, 3, 4, 1, 5).reshape(N_GRP, N_BOX, NCOL, FIELDS, CZ)
    low_sum = face_low.reshape(N_GRP, FIELDS, FY // 2, 2, CZ, 2).sum(axis=(3, 5)).transpose(0, 2, 1, 3)
    high_sum = face_high.reshape(N_GRP, FIELDS, FY // 2, 2, CZ, 2).sum(axis=(3, 5)).transpose(0, 2, 1, 3)
    low_term = -time_step / 8 * low_sum
    high_term = time_step / 8 * high_sum
    box_ids = jnp.arange(N_BOX, dtype=jnp.int32)[None, :, None, None, None]
    flux_records = jnp.where(box_ids == 0, low_term[:, None], jnp.where(box_ids == N_BOX - 1, high_term[:, None], 0.0))
    payload = jnp.concatenate([avg_records, flux_records], axis=2)
    record_ids = jnp.arange(REC, dtype=jnp.int32)[None, None, :]
    box_index = jnp.broadcast_to(jnp.arange(N_BOX, dtype=jnp.int32)[None, :, None], (N_GRP, N_BOX, REC))
    is_average = jnp.broadcast_to(record_ids < NCOL, (N_GRP, N_BOX, REC))
    end_box = (box_index == 0) | (box_index == N_BOX - 1)
    is_face = (record_ids >= NCOL) & end_box
    is_live = is_average | is_face
    values = jnp.zeros((N_GRP, N_BOX, REC, FIELDS, CZ), jnp.float32).at[dest_grp, box_index, dest_column].add(jnp.where(is_live[..., None, None], payload, 0.0))
    avg_flag = jnp.zeros((N_GRP, N_BOX, REC), jnp.float32).at[dest_grp, box_index, dest_column].add(is_average.astype(jnp.float32))
    face_flag = jnp.zeros((N_GRP, N_BOX, REC), jnp.float32).at[dest_grp, box_index, dest_column].add(is_face.astype(jnp.float32))
    coarse_new = jnp.where(avg_flag[..., None, None] > 0, values, coarse_state + face_flag[..., None, None] * (values - coarse_face_term))
    return (fine_new, coarse_new)
```

```python
import functools

import jax
import jax.numpy as jnp
from jax import lax
from jax.experimental import pallas as pl
from jax.experimental.pallas import tpu as pltpu
from jax.sharding import PartitionSpec as P

gamma_ratio = 1.4
time_step = 0.06
vmem_limit = 8 * 1024 * 1024


def split_dot(lhs, rhs, split_lhs, dims=(((1,), (0,)), ((), ()))):
    data = lhs if split_lhs else rhs
    exact = (rhs if split_lhs else lhs).astype(jnp.bfloat16)
    total = None
    for _ in range(3):
        term = data.astype(jnp.bfloat16)
        data = data - term.astype(jnp.float32)
        pair = (term, exact) if split_lhs else (exact, term)
        part = lax.dot_general(*pair, dims, preferred_element_type=jnp.float32)
        total = part if total is None else total + part
    return total


def next_z(values):
    return pltpu.roll(values, values.shape[-1] - 1, 1)


def last_z(values):
    return pltpu.roll(values, 1, 1)


def next_y(pair):
    even, odd = pair
    return (odd, pltpu.roll(even, even.shape[0] - 1, 0))


def last_y(pair):
    even, odd = pair
    return (pltpu.roll(odd, 1, 0), even)


def both(function, *pairs):
    return tuple(function(*halves) for halves in zip(*pairs))


class Cells:

    def __init__(self, state):
        density, mom = state[0], state[1:4]
        inverse = both(lambda d: 1.0 / d, density)
        velocity = [both(lambda m, r: m * r, m, inverse) for m in mom]
        square = {}
        for i in range(3):
            for j in range(i, 3):
                square[i, j] = both(lambda m, v: m * v, mom[i], velocity[j])
        pressure = both(
            lambda e, a, b, c: (gamma_ratio - 1.0) * (e - 0.5 * (a + b + c)),
            state[4], square[0, 0], square[1, 1], square[2, 2],
        )
        sound = both(lambda p, r: jnp.sqrt(gamma_ratio * p * r), pressure, inverse)
        enthalpy = both(jnp.add, state[4], pressure)
        self.state = state
        self.flux = []
        self.speed = []
        for normal in range(3):
            pieces = [mom[normal]]
            for member in range(3):
                term = square[min(member, normal), max(member, normal)]
                pieces.append(both(jnp.add, term, pressure) if member == normal else term)
            pieces.append(both(jnp.multiply, enthalpy, velocity[normal]))
            self.flux.append(pieces)
            self.speed.append(both(lambda v, c: jnp.abs(v) + c, velocity[normal], sound))


def doubled_face(left_state, right_state, left_flux, right_flux, left_speed, right_speed):
    biggest = both(jnp.maximum, left_speed, right_speed)
    return [
        both(lambda a, b, f, g, s: (f + g) - s * (b - a), ls, rs, lf, rf, biggest)
        for ls, rs, lf, rf in zip(left_state, right_state, left_flux, right_flux)
    ]


def x_face(left, right):
    return doubled_face(
        left.state, right.state, left.flux[0], right.flux[0], left.speed[0], right.speed[0]
    )


def side_change(cells):
    change = [None] * len(cells.state)
    for normal in (1, 2):
        if normal == 1:
            ahead, behind = next_y, last_y
        else:
            ahead = functools.partial(both, next_z)
            behind = functools.partial(both, last_z)
        faces = doubled_face(
            cells.state, [ahead(s) for s in cells.state],
            cells.flux[normal], [ahead(f) for f in cells.flux[normal]],
            cells.speed[normal], ahead(cells.speed[normal]),
        )
        for index, face in enumerate(faces):
            part = both(jnp.subtract, face, behind(face))
            change[index] = part if change[index] is None else both(jnp.add, change[index], part)
    return change


def advance(layers, on_update, on_face):
    before, low_face, change = Cells(layers[0]()), None, None
    for index in range(1, len(layers)):
        here = Cells(layers[index]())
        face = x_face(before, here)
        on_face(index - 1, face)
        if index >= 2:
            half = 0.5 * time_step
            on_update(
                index - 1,
                [
                    both(lambda u, c, h, l: u - half * (c + (h - l)), u, c, h, l)
                    for u, c, h, l in zip(before.state, change, face, low_face)
                ],
            )
        if index < len(layers) - 1:
            change = side_change(here)
        before, low_face = here, face


def one_hot_slots(owners, groups, capacity):
    total = owners.shape[1]
    hit = owners == lax.broadcasted_iota(jnp.int32, (groups, total), 0)
    hot = jnp.where(hit, 1.0, 0.0)
    earlier = (
        lax.broadcasted_iota(jnp.int32, (total, total), 0)
        < lax.broadcasted_iota(jnp.int32, (total, total), 1)
    )
    rank = jnp.dot(
        hot.astype(jnp.bfloat16),
        jnp.where(earlier, 1.0, 0.0).astype(jnp.bfloat16),
        preferred_element_type=jnp.float32,
    )
    return [jnp.where(hit & (rank == float(slot)), 1.0, 0.0) for slot in range(capacity)]


def patch_kernel(
    box_count, groups, capacity, rows,
    box_ref, fine_ref, ghost_ref, low_ref, high_ref, owner_ref, column_ref,
    new_ref, out_ref, half_ref, stage_ref,
):
    box_place = box_ref[0]
    at_low = box_place == 0
    at_high = box_place == box_count - 1
    fields, along, across, depth = fine_ref.shape
    half_across = across // 2
    lanes = stage_ref.shape[-1]
    pieces = depth // lanes
    mirrored = box_count == 2
    side = jnp.where(at_high, 1, 0) if mirrored else 0
    turn = jnp.where(at_high, -1.0, 1.0)

    def place(index):
        return jnp.where(at_high, along - 1 - index, index) if mirrored else index

    def oriented(field, values):
        return turn * values if mirrored and field == 1 else values

    slots = iter(range(stage_ref.shape[0]))

    def parted(planes):
        slot = next(slots)
        for f, plane in enumerate(planes):
            for piece in range(pieces):
                stage_ref[slot, f, piece] = oriented(f, plane[:, piece * lanes:(piece + 1) * lanes])
        return [
            tuple(
                jnp.concatenate(
                    [
                        stage_ref[slot, f, piece, pl.ds(parity, half_across, stride=2), :]
                        for piece in range(pieces)
                    ],
                    axis=1,
                )
                for parity in (0, 1)
            )
            for f in range(fields)
        ]

    def rows_of(ref, layer):
        return parted([ref[f, layer] for f in range(fields)])

    def ghost_layer(at, time_frac):
        if time_frac == 0.0:
            return parted([ghost_ref[0, at, f] for f in range(fields)])
        return parted(
            [
                (1.0 - time_frac) * ghost_ref[0, at, f] + time_frac * ghost_ref[1, at, f]
                for f in range(fields)
            ]
        )

    def half_layer(index):
        return [tuple(half_ref[index, f, parity] for parity in (0, 1)) for f in range(fields)]

    def picked(flag, first, second):
        return [both(lambda a, b: jnp.where(flag, a, b), a, b) for a, b in zip(first, second)]

    def fine_layer(index):
        return rows_of(fine_ref, place(index))

    inner = [functools.partial(fine_layer, index) for index in range(along)]
    low_faces, high_faces = [], []
    if mirrored:
        start = 0
        first = [lambda: ghost_layer(side, 0.0), *inner]
        first += [lambda: rows_of(low_ref, place(0)), lambda: rows_of(low_ref, place(1))]
        second = [lambda: ghost_layer(side, 0.5)]
        second += [functools.partial(half_layer, index) for index in range(along + 1)]
        low_at = (0, 0)
        high_at = (-1, -1)
    else:
        start = 1
        width = low_ref.shape[1]
        first = [lambda: rows_of(low_ref, width - 2)]
        first += [
            lambda: picked(at_low, ghost_layer(0, 0.0), rows_of(low_ref, width - 1)),
            *inner,
            lambda: picked(at_high, ghost_layer(1, 0.0), rows_of(high_ref, 0)),
            lambda: rows_of(high_ref, 1),
        ]
        second = [lambda: picked(at_low, ghost_layer(0, 0.5), half_layer(0))]
        second += [functools.partial(half_layer, 1 + index) for index in range(along)]
        second += [lambda: picked(at_high, ghost_layer(1, 0.5), half_layer(along + 1))]
        low_at = (1, 0)
        high_at = (along + 1, along)

    def keep_half(index, state):
        for f in range(fields):
            for parity in (0, 1):
                half_ref[index - 1, f, parity] = state[f][parity]

    sums = {}

    def keep_new(index, state):
        slot = next(slots)
        layer = place(index - 1)
        for f in range(fields):
            for piece in range(pieces):
                part = slice(piece * lanes, (piece + 1) * lanes)
                for parity in (0, 1):
                    stage_ref[slot, f, piece, pl.ds(parity, half_across, stride=2), :] = oriented(
                        f, state[f][parity][:, part]
                    )
                new_ref[f, layer, :, part] = stage_ref[slot, f, piece]
            pooled = state[f][0] + state[f][1]
            key = (f, (index - 1) // 2)
            sums[key] = sums[key] + pooled if key in sums else pooled

    def face_keeper(step):
        def keep(index, face):
            if index == low_at[step]:
                low_faces.append(face)
            if index == high_at[step]:
                high_faces.append(face)
        return keep

    advance(first, keep_half, face_keeper(0))
    advance(second, keep_new, face_keeper(1))

    planes = along // 2
    blocks = []
    for f in range(fields):
        for plane in range(planes):
            if mirrored:
                value = jnp.where(at_high, sums[f, planes - 1 - plane], sums[f, plane])
            else:
                value = sums[f, plane]
            blocks.append(oriented(f, 0.125 * value))
        low = [sum(halves) for halves in zip(*(step[f] for step in low_faces))]
        face_sum = low[0] + low[1]
        if not mirrored:
            high = [sum(halves) for halves in zip(*(step[f] for step in high_faces))]
            face_sum = jnp.where(at_low, face_sum, -(high[0] + high[1]))
        blocks.append(oriented(f, (-0.5 * time_step / 8) * face_sum))
    stacked = jnp.concatenate(blocks, axis=0)
    coarse_depth = depth // 2
    lane_pair = lax.broadcasted_iota(jnp.int32, (depth, coarse_depth), 0) // 2
    pool = jnp.where(
        lane_pair == lax.broadcasted_iota(jnp.int32, (depth, coarse_depth), 1), 1.0, 0.0
    )
    records = split_dot(stacked, pool, True)

    total = owner_ref.shape[1]
    count_average = planes * half_across
    selections = one_hot_slots(owner_ref[...], groups, capacity)
    wide = jnp.concatenate(
        [records[f * total:(f + 1) * total] for f in range(fields)], axis=1
    )
    chosen = split_dot(jnp.concatenate(selections, axis=0), wide, False)
    record_ids = lax.broadcasted_iota(jnp.int32, (1, total), 1)
    codes = (column_ref[...] + 1).astype(jnp.float32)
    face_code = -codes if mirrored else jnp.where(at_low | at_high, -codes, 0.0)
    codes = jnp.where(record_ids < count_average, codes, face_code)
    for slot in range(capacity):
        base = slot * (fields + 1)
        for f in range(fields):
            out_ref[pl.ds(base + f, groups, stride=rows), :] = chosen[
                slot * groups:(slot + 1) * groups, f * coarse_depth:(f + 1) * coarse_depth
            ]
        code = jnp.sum(selections[slot] * codes, axis=1, keepdims=True)
        out_ref[pl.ds(base + fields, groups, stride=rows), :] = jnp.broadcast_to(
            code, (groups, coarse_depth)
        )


def owner_kernel(groups, capacity, rows, in_ref, state_ref, term_ref, out_ref):
    fields, total, coarse_depth = state_ref.shape
    codes, values = [], []
    for slot in range(capacity):
        base = slot * (fields + 1)
        code = in_ref[pl.ds(base + fields, groups, stride=rows), :]
        codes.append(code)
        values.append(
            jnp.concatenate(
                [
                    jnp.where(code != 0.0, in_ref[pl.ds(base + f, groups, stride=rows), :], 0.0)
                    for f in range(fields)
                ],
                axis=1,
            )
        )
    codes = jnp.concatenate(codes, axis=0)
    values = jnp.concatenate(values, axis=0)
    count = codes.shape[0]
    across = jnp.transpose(codes)[:total]
    column = (lax.broadcasted_iota(jnp.int32, (total, count), 0) + 1).astype(jnp.float32)
    hot = jnp.where(jnp.abs(across) == column, 1.0, 0.0)
    kind = jnp.where(codes > 0.0, 1.0, jnp.where(codes < 0.0, -1.0, 0.0))
    flag = jnp.dot(
        hot.astype(jnp.bfloat16), kind.astype(jnp.bfloat16), preferred_element_type=jnp.float32
    )
    got = split_dot(hot, values, False)
    for f in range(fields):
        value = got[:, f * coarse_depth:(f + 1) * coarse_depth]
        state = state_ref[f]
        refluxed = state + (value - term_ref[f])
        out_ref[f] = jnp.where(flag > 0.0, value, jnp.where(flag < 0.0, refluxed, state))


def on_device(fine_state, patch_ghosts, coarse_state, coarse_face_term, dest_grp, dest_column):
    box_count = lax.axis_size("box")
    group_count = lax.axis_size("grp")
    box_place = lax.axis_index("box")
    current = fine_state[0]
    fields, cells_along, cells_across, cells_depth = current.shape
    total = dest_grp.shape[-1]
    capacity = (total + group_count - 1) // group_count
    rows = -(-capacity * (fields + 1) // 8) * 8
    coarse_depth = cells_depth // 2
    params = pltpu.CompilerParams(vmem_limit_bytes=vmem_limit)

    if box_count == 2:
        low = lax.ppermute(current, "box", [(0, 1), (1, 0)])
        high = low
    else:
        ends = box_count - 1
        low = lax.ppermute(current[:, -2:], "box", [(i, i + 1) for i in range(ends)])
        high = lax.ppermute(current[:, :2], "box", [(i + 1, i) for i in range(ends)])

    vmem = pl.BlockSpec(memory_space=pltpu.VMEM)
    halves = cells_along + (1 if box_count == 2 else 2)
    updated, outgoing = pl.pallas_call(
        functools.partial(patch_kernel, box_count, group_count, capacity, rows),
        out_shape=(
            jax.ShapeDtypeStruct(current.shape, jnp.float32),
            jax.ShapeDtypeStruct((group_count * rows, coarse_depth), jnp.float32),
        ),
        in_specs=[pl.BlockSpec(memory_space=pltpu.SMEM)] + [vmem] * 6,
        out_specs=(vmem, vmem),
        scratch_shapes=[
            pltpu.VMEM((halves, fields, 2, cells_across // 2, cells_depth), jnp.float32),
            pltpu.VMEM(
                (2 * cells_along + 8, fields, cells_depth // 128, cells_across, 128), jnp.float32
            ),
        ],
        compiler_params=params,
        name="patch",
    )(
        box_place.reshape(1), current, patch_ghosts[0], low, high,
        dest_grp[0], dest_column[0],
    )
    incoming = lax.all_to_all(
        outgoing.reshape(group_count, rows, coarse_depth),
        "grp", split_axis=0, concat_axis=0, tiled=True,
    ).reshape(group_count * rows, coarse_depth)
    coarse_new = pl.pallas_call(
        functools.partial(owner_kernel, group_count, capacity, rows),
        out_shape=jax.ShapeDtypeStruct((fields, total, coarse_depth), jnp.float32),
        in_specs=[vmem] * 3,
        out_specs=vmem,
        compiler_params=params,
        name="owner",
    )(
        incoming,
        coarse_state[0, 0].transpose(1, 0, 2),
        coarse_face_term[0, 0].transpose(1, 0, 2),
    )
    return (updated[None], coarse_new.transpose(1, 0, 2)[None, None])


def solution(mesh):
    in_specs = (
        P("grp", None, "box", None, None),
        P("grp", None, None, None, None, None),
        P("grp", "box", None, None, None),
        P("grp", "box", None, None, None),
        P("grp", "box", None),
        P("grp", "box", None),
    )
    out_specs = (P("grp", None, "box", None, None), P("grp", "box", None, None, None))
    return jax.shard_map(
        on_device, mesh=mesh, in_specs=in_specs, out_specs=out_specs, check_vma=False
    )
```

```python
import functools

import jax
import jax.numpy as jnp
from jax import lax
from jax.experimental import pallas as pl
from jax.experimental.pallas import tpu as pltpu
from jax.sharding import PartitionSpec as P

gamma_ratio = 1.4
time_step = 0.06
vmem_limit = 8 * 1024 * 1024


def split_dot(lhs, rhs, split_lhs, dims=(((1,), (0,)), ((), ()))):
    data = lhs if split_lhs else rhs
    exact = (rhs if split_lhs else lhs).astype(jnp.bfloat16)
    total = None
    for _ in range(3):
        term = data.astype(jnp.bfloat16)
        data = data - term.astype(jnp.float32)
        pair = (term, exact) if split_lhs else (exact, term)
        part = lax.dot_general(*pair, dims, preferred_element_type=jnp.float32)
        total = part if total is None else total + part
    return total


def next_z(values):
    return pltpu.roll(values, values.shape[-1] - 1, 1)


def last_z(values):
    return pltpu.roll(values, 1, 1)


def next_y(pair):
    even, odd = pair
    return (odd, pltpu.roll(even, even.shape[0] - 1, 0))


def last_y(pair):
    even, odd = pair
    return (pltpu.roll(odd, 1, 0), even)


def both(function, *pairs):
    return tuple(function(*halves) for halves in zip(*pairs))


class Cells:

    def __init__(self, state):
        density, mom = state[0], state[1:4]
        inverse = both(lambda d: 1.0 / d, density)
        velocity = [both(lambda m, r: m * r, m, inverse) for m in mom]
        square = {}
        for i in range(3):
            for j in range(i, 3):
                square[i, j] = both(lambda m, v: m * v, mom[i], velocity[j])
        pressure = both(
            lambda e, a, b, c: (gamma_ratio - 1.0) * (e - 0.5 * (a + b + c)),
            state[4], square[0, 0], square[1, 1], square[2, 2],
        )
        sound = both(lambda p, r: jnp.sqrt(gamma_ratio * p * r), pressure, inverse)
        enthalpy = both(jnp.add, state[4], pressure)
        self.state = state
        self.flux = []
        self.speed = []
        for normal in range(3):
            pieces = [mom[normal]]
            for member in range(3):
                term = square[min(member, normal), max(member, normal)]
                pieces.append(both(jnp.add, term, pressure) if member == normal else term)
            pieces.append(both(jnp.multiply, enthalpy, velocity[normal]))
            self.flux.append(pieces)
            self.speed.append(both(lambda v, c: jnp.abs(v) + c, velocity[normal], sound))


def doubled_face(left_state, right_state, left_flux, right_flux, left_speed, right_speed):
    biggest = both(jnp.maximum, left_speed, right_speed)
    return [
        both(lambda a, b, f, g, s: (f + g) - s * (b - a), ls, rs, lf, rf, biggest)
        for ls, rs, lf, rf in zip(left_state, right_state, left_flux, right_flux)
    ]


def x_face(left, right):
    return doubled_face(
        left.state, right.state, left.flux[0], right.flux[0], left.speed[0], right.speed[0]
    )


def side_change(cells):
    change = [None] * len(cells.state)
    for normal in (1, 2):
        if normal == 1:
            ahead, behind = next_y, last_y
        else:
            ahead = functools.partial(both, next_z)
            behind = functools.partial(both, last_z)
        faces = doubled_face(
            cells.state, [ahead(s) for s in cells.state],
            cells.flux[normal], [ahead(f) for f in cells.flux[normal]],
            cells.speed[normal], ahead(cells.speed[normal]),
        )
        for index, face in enumerate(faces):
            part = both(jnp.subtract, face, behind(face))
            change[index] = part if change[index] is None else both(jnp.add, change[index], part)
    return change


def advance(layers, on_update, on_face):
    before, low_face, change = Cells(layers[0]()), None, None
    for index in range(1, len(layers)):
        here = Cells(layers[index]())
        face = x_face(before, here)
        on_face(index - 1, face)
        if index >= 2:
            half = 0.5 * time_step
            on_update(
                index - 1,
                [
                    both(lambda u, c, h, l: u - half * (c + (h - l)), u, c, h, l)
                    for u, c, h, l in zip(before.state, change, face, low_face)
                ],
            )
        if index < len(layers) - 1:
            change = side_change(here)
        before, low_face = here, face


def step_state(state, change, high_face, low_face):
    half = 0.5 * time_step
    return [
        both(lambda u, c, h, l: u - half * (c + (h - l)), u, c, h, l)
        for u, c, h, l in zip(state, change, high_face, low_face)
    ]


def split_z(ref, slot, field, half_across):
    return tuple(
        jnp.concatenate(
            [
                ref[slot, field, piece, pl.ds(parity, half_across, stride=2), :]
                for piece in range(ref.shape[2])
            ],
            axis=1,
        )
        for parity in (0, 1)
    )


def put_layer(stage_ref, slot, new_ref, layer, state, turn):
    fields, pieces, _, lanes = stage_ref.shape[1:]
    half_across = state[0][0].shape[0]
    for f in range(fields):
        for piece in range(pieces):
            part = slice(piece * lanes, (piece + 1) * lanes)
            for parity in (0, 1):
                values = state[f][parity][:, part]
                stage_ref[slot, f, piece, pl.ds(parity, half_across, stride=2), :] = (
                    turn * values if f == 1 else values
                )
            new_ref[f, layer, :, part] = stage_ref[slot, f, piece]


class Carried:

    def __init__(self, ref, slot, fields):
        def pair(index):
            return tuple(ref[slot, index, parity] for parity in (0, 1))

        self.state = [pair(f) for f in range(fields)]
        self.flux = [[self.state[1]] + [pair(fields + f) for f in range(1, fields)]]
        self.speed = [pair(fields)]
        self.partial = [pair(2 * fields + f) for f in range(fields)]

    @staticmethod
    def keep(ref, slot, cells, change, low_face):
        half = 0.5 * time_step
        fields = len(cells.state)
        for f in range(fields):
            for parity in (0, 1):
                ref[slot, f, parity] = cells.state[f][parity]
                ref[slot, 2 * fields + f, parity] = cells.state[f][parity] - half * (
                    change[f][parity] - low_face[f][parity]
                )
                ref[slot, fields + f, parity] = (
                    cells.flux[0][f][parity] if f > 0 else cells.speed[0][parity]
                )

    def finished(self, high_face):
        half = 0.5 * time_step
        return [both(lambda p, h: p - half * h, p, h) for p, h in zip(self.partial, high_face)]


def early_kernel(
    groups, capacity, fine_ref, ghost_ref, owner_ref, column_ref,
    new_ref, carry_ref, face_ref, sum_ref, select_ref, code_ref,
    stage_ref, owner_vmem, column_vmem, copy_sems,
):
    _, fields, along, across, depth = fine_ref.shape
    half_across = across // 2
    lanes = stage_ref.shape[-1]
    pieces = depth // lanes
    at_high = lax.axis_index("box") == 1
    side = jnp.where(at_high, 1, 0)
    turn = jnp.where(at_high, -1.0, 1.0)

    copies = {}

    def fetch(slot, source):
        for piece in range(pieces):
            copies[slot, piece] = pltpu.make_async_copy(
                source(slice(piece * lanes, (piece + 1) * lanes)),
                stage_ref.at[slot, :, piece],
                copy_sems.at[slot * pieces + piece],
            )
            copies[slot, piece].start()

    ghost_slots = (0, along + 1)
    fetch(0, lambda part: ghost_ref.at[0, 0, side, :, :, part])
    for index in range(along):
        layer = jnp.where(at_high, along - 1 - index, index)
        fetch(1 + index, lambda part, layer=layer: fine_ref.at[0, :, layer, :, part])
    fetch(along + 1, lambda part: ghost_ref.at[0, 1, side, :, :, part])
    small = [
        pltpu.make_async_copy(owner_ref, owner_vmem, copy_sems.at[(along + 2) * pieces]),
        pltpu.make_async_copy(column_ref, column_vmem, copy_sems.at[(along + 2) * pieces + 1]),
    ]
    for copy in small:
        copy.start()

    def arrived(slot):
        for piece in range(pieces):
            copies[slot, piece].wait()
        planes = [split_z(stage_ref, slot, f, half_across) for f in range(fields)]
        planes[1] = tuple(turn * values for values in planes[1])
        return planes

    ghost_now = arrived(0)
    before, low_face, change = Cells(ghost_now), None, None
    faces = []
    halves = []
    for index in range(along):
        here = Cells(arrived(1 + index))
        face = x_face(before, here)
        if index == 0:
            faces.append(face)
        else:
            halves.append(step_state(before.state, change, face, low_face))
        change = side_change(here)
        before, low_face = here, face
    Carried.keep(carry_ref, 0, before, change, low_face)

    ghost_end = arrived(along + 1)
    before = Cells(
        [both(lambda a, b: 0.5 * a + 0.5 * b, a, b) for a, b in zip(ghost_now, ghost_end)]
    )
    low_face, change = None, None
    total_sums = {}
    for index in range(along - 1):
        here = Cells(halves[index])
        face = x_face(before, here)
        if index == 0:
            faces.append(face)
        else:
            state = step_state(before.state, change, face, low_face)
            layer = jnp.where(at_high, along - index, index - 1)
            put_layer(stage_ref, along + 1 + index, new_ref, layer, state, turn)
            for f in range(fields):
                key = (index - 1) // 2, f
                pooled = state[f][0] + state[f][1]
                total_sums[key] = total_sums[key] + pooled if key in total_sums else pooled
        change = side_change(here)
        before, low_face = here, face
    Carried.keep(carry_ref, 1, before, change, low_face)
    for (plane, f), pooled in total_sums.items():
        sum_ref[plane, f] = pooled
    for f in range(fields):
        both_steps = [faces[0][f][parity] + faces[1][f][parity] for parity in (0, 1)]
        face_ref[f] = both_steps[0] + both_steps[1]

    for copy in small:
        copy.wait()
    total = owner_vmem.shape[1]
    count_average = (along // 2) * half_across
    selections = one_hot_slots(owner_vmem[...], groups, capacity)
    record_ids = lax.broadcasted_iota(jnp.int32, (1, total), 1)
    codes = (column_vmem[...] + 1).astype(jnp.float32)
    codes = jnp.where(record_ids < count_average, codes, -codes)
    for slot in range(capacity):
        rows = slice(slot * groups, (slot + 1) * groups)
        select_ref[rows] = selections[slot]
        code = jnp.sum(selections[slot] * codes, axis=1, keepdims=True)
        code_ref[rows] = jnp.broadcast_to(code, (groups, code_ref.shape[1]))


def late_kernel(
    groups, capacity, rows, carry_ref, other_ref, face_ref, sum_ref, select_ref, code_ref,
    early_ref, new_ref, out_ref, stage_ref,
):
    del early_ref
    fields, along, across, depth = other_ref.shape
    half_across = across // 2
    lanes = stage_ref.shape[-1]
    pieces = depth // lanes
    at_high = lax.axis_index("box") == 1
    turn = jnp.where(at_high, -1.0, 1.0)

    def place(index):
        return jnp.where(at_high, along - 1 - index, index)

    def received(index):
        for f in range(fields):
            plane = other_ref[f, place(index)]
            for piece in range(pieces):
                stage_ref[index, f, piece] = plane[:, piece * lanes:(piece + 1) * lanes]
        planes = [split_z(stage_ref, index, f, half_across) for f in range(fields)]
        planes[1] = tuple(turn * values for values in planes[1])
        return planes

    near = Cells(received(0))
    end = Carried(carry_ref, 0, fields)
    end_face = x_face(end, near)
    end_half = end.finished(end_face)
    near_half = step_state(
        near.state, side_change(near), x_face(near, Cells(received(1))), end_face
    )
    inner = Carried(carry_ref, 1, fields)
    last = Cells(end_half)
    inner_face = x_face(inner, last)
    inner_new = inner.finished(inner_face)
    last_new = step_state(
        last.state, side_change(last), x_face(last, Cells(near_half)), inner_face
    )
    put_layer(stage_ref, 2, new_ref, place(along - 2), inner_new, turn)
    put_layer(stage_ref, 3, new_ref, place(along - 1), last_new, turn)

    planes = along // 2
    blocks = []
    for f in range(fields):
        sums = [sum_ref[plane, f] for plane in range(planes - 1)]
        sums.append(
            (inner_new[f][0] + inner_new[f][1]) + (last_new[f][0] + last_new[f][1])
        )
        scale = turn if f == 1 else 1.0
        for plane in range(planes):
            blocks.append(
                (0.125 * scale) * jnp.where(at_high, sums[planes - 1 - plane], sums[plane])
            )
        blocks.append((-0.5 * time_step / 8 * scale) * face_ref[f])
    route(
        jnp.concatenate(blocks, axis=0), select_ref[...], groups, capacity, rows, fields, out_ref
    )
    for slot in range(capacity):
        out_ref[pl.ds(slot * (fields + 1) + fields, groups, stride=rows), :] = code_ref[
            slot * groups:(slot + 1) * groups
        ]


def route(stacked, selection, groups, capacity, rows, fields, out_ref):
    depth, coarse_depth = stacked.shape[1], out_ref.shape[1]
    lane_pair = lax.broadcasted_iota(jnp.int32, (depth, coarse_depth), 0) // 2
    pool = jnp.where(
        lane_pair == lax.broadcasted_iota(jnp.int32, (depth, coarse_depth), 1), 1.0, 0.0
    )
    records = split_dot(stacked, pool, True)
    total = records.shape[0] // fields
    wide = jnp.concatenate(
        [records[f * total:(f + 1) * total] for f in range(fields)], axis=1
    )
    chosen = split_dot(selection, wide, False)
    for slot in range(capacity):
        for f in range(fields):
            out_ref[pl.ds(slot * (fields + 1) + f, groups, stride=rows), :] = chosen[
                slot * groups:(slot + 1) * groups, f * coarse_depth:(f + 1) * coarse_depth
            ]


def one_hot_slots(owners, groups, capacity):
    total = owners.shape[1]
    hit = owners == lax.broadcasted_iota(jnp.int32, (groups, total), 0)
    hot = jnp.where(hit, 1.0, 0.0)
    earlier = (
        lax.broadcasted_iota(jnp.int32, (total, total), 0)
        < lax.broadcasted_iota(jnp.int32, (total, total), 1)
    )
    rank = jnp.dot(
        hot.astype(jnp.bfloat16),
        jnp.where(earlier, 1.0, 0.0).astype(jnp.bfloat16),
        preferred_element_type=jnp.float32,
    )
    return [jnp.where(hit & (rank == float(slot)), 1.0, 0.0) for slot in range(capacity)]


def patch_kernel(
    box_count, groups, capacity, rows,
    fine_ref, ghost_ref, low_ref, high_ref, owner_ref, column_ref,
    new_ref, out_ref, half_ref, stage_ref,
):
    box_place = lax.axis_index("box")
    at_low = box_place == 0
    at_high = box_place == box_count - 1
    fields, along, across, depth = fine_ref.shape
    half_across = across // 2
    lanes = stage_ref.shape[-1]
    pieces = depth // lanes
    slots = iter(range(stage_ref.shape[0]))

    def parted(planes):
        slot = next(slots)
        for f, plane in enumerate(planes):
            for piece in range(pieces):
                stage_ref[slot, f, piece] = plane[:, piece * lanes:(piece + 1) * lanes]
        return [split_z(stage_ref, slot, f, half_across) for f in range(fields)]

    def rows_of(ref, layer):
        return parted([ref[f, layer] for f in range(fields)])

    def ghost_layer(at, time_frac):
        return parted(
            [
                (1.0 - time_frac) * ghost_ref[0, at, f] + time_frac * ghost_ref[1, at, f]
                for f in range(fields)
            ]
        )

    def half_layer(index):
        return [tuple(half_ref[index, f, parity] for parity in (0, 1)) for f in range(fields)]

    def picked(flag, first, second):
        return [both(lambda a, b: jnp.where(flag, a, b), a, b) for a, b in zip(first, second)]

    width = low_ref.shape[1]
    first = [lambda: rows_of(low_ref, width - 2)]
    first += [lambda: picked(at_low, ghost_layer(0, 0.0), rows_of(low_ref, width - 1))]
    first += [functools.partial(rows_of, fine_ref, index) for index in range(along)]
    first += [lambda: picked(at_high, ghost_layer(1, 0.0), rows_of(high_ref, 0))]
    first += [lambda: rows_of(high_ref, 1)]
    second = [lambda: picked(at_low, ghost_layer(0, 0.5), half_layer(0))]
    second += [functools.partial(half_layer, 1 + index) for index in range(along)]
    second += [lambda: picked(at_high, ghost_layer(1, 0.5), half_layer(along + 1))]
    low_at, high_at = (1, 0), (along + 1, along)
    low_faces, high_faces, sums = [], [], {}

    def keep_half(index, state):
        for f in range(fields):
            for parity in (0, 1):
                half_ref[index - 1, f, parity] = state[f][parity]

    def keep_new(index, state):
        put_layer(stage_ref, next(slots), new_ref, index - 1, state, 1.0)
        for f in range(fields):
            pooled = state[f][0] + state[f][1]
            key = (f, (index - 1) // 2)
            sums[key] = sums[key] + pooled if key in sums else pooled

    def face_keeper(step):
        def keep(index, face):
            if index == low_at[step]:
                low_faces.append(face)
            if index == high_at[step]:
                high_faces.append(face)
        return keep

    advance(first, keep_half, face_keeper(0))
    advance(second, keep_new, face_keeper(1))

    planes = along // 2
    blocks = []
    for f in range(fields):
        blocks += [0.125 * sums[f, plane] for plane in range(planes)]
        low = [low_faces[0][f][parity] + low_faces[1][f][parity] for parity in (0, 1)]
        high = [high_faces[0][f][parity] + high_faces[1][f][parity] for parity in (0, 1)]
        face_sum = jnp.where(at_low, low[0] + low[1], -(high[0] + high[1]))
        blocks.append((-0.5 * time_step / 8) * face_sum)
    total = owner_ref.shape[1]
    selections = one_hot_slots(owner_ref[...], groups, capacity)
    route(
        jnp.concatenate(blocks, axis=0), jnp.concatenate(selections, axis=0),
        groups, capacity, rows, fields, out_ref,
    )
    record_ids = lax.broadcasted_iota(jnp.int32, (1, total), 1)
    codes = (column_ref[...] + 1).astype(jnp.float32)
    face_code = jnp.where(at_low | at_high, -codes, 0.0)
    codes = jnp.where(record_ids < planes * half_across, codes, face_code)
    for slot in range(capacity):
        code = jnp.sum(selections[slot] * codes, axis=1, keepdims=True)
        out_ref[pl.ds(slot * (fields + 1) + fields, groups, stride=rows), :] = jnp.broadcast_to(
            code, (groups, out_ref.shape[1])
        )


def owner_kernel(
    groups, capacity, rows, in_ref, state_ref, term_ref, new_ref,
    coarse_ref, final_ref, out_ref, copy_sems,
):
    write_fine = pltpu.make_async_copy(new_ref, final_ref, copy_sems.at[0])
    write_fine.start()
    fields, total, coarse_depth = state_ref.shape
    codes, values = [], []
    for slot in range(capacity):
        base = slot * (fields + 1)
        code = in_ref[pl.ds(base + fields, groups, stride=rows), :]
        codes.append(code)
        values.append(
            jnp.concatenate(
                [
                    jnp.where(code != 0.0, in_ref[pl.ds(base + f, groups, stride=rows), :], 0.0)
                    for f in range(fields)
                ],
                axis=1,
            )
        )
    codes = jnp.concatenate(codes, axis=0)
    values = jnp.concatenate(values, axis=0)
    count = codes.shape[0]
    across = jnp.transpose(codes)[:total]
    column = (lax.broadcasted_iota(jnp.int32, (total, count), 0) + 1).astype(jnp.float32)
    hot = jnp.where(jnp.abs(across) == column, 1.0, 0.0)
    kind = jnp.where(codes > 0.0, 1.0, jnp.where(codes < 0.0, -1.0, 0.0))
    flag = jnp.dot(
        hot.astype(jnp.bfloat16), kind.astype(jnp.bfloat16), preferred_element_type=jnp.float32
    )
    got = split_dot(hot, values, False)
    for f in range(fields):
        value = got[:, f * coarse_depth:(f + 1) * coarse_depth]
        state = state_ref[f]
        refluxed = state + (value - term_ref[f])
        out_ref[f] = jnp.where(flag > 0.0, value, jnp.where(flag < 0.0, refluxed, state))
    write_coarse = pltpu.make_async_copy(out_ref, coarse_ref, copy_sems.at[1])
    write_coarse.start()
    write_fine.wait()
    write_coarse.wait()


def on_device(fine_state, patch_ghosts, coarse_state, coarse_face_term, dest_grp, dest_column):
    box_count = lax.axis_size("box")
    group_count = lax.axis_size("grp")
    current = fine_state[0]
    fields, cells_along, cells_across, cells_depth = current.shape
    total = dest_grp.shape[-1]
    capacity = (total + group_count - 1) // group_count
    rows = -(-capacity * (fields + 1) // 8) * 8
    coarse_depth = cells_depth // 2
    params = pltpu.CompilerParams(vmem_limit_bytes=vmem_limit)
    vmem = pl.BlockSpec(memory_space=pltpu.VMEM)
    hbm = pl.BlockSpec(memory_space=pltpu.HBM)
    half_across, pieces = cells_across // 2, cells_depth // 128
    outgoing_shape = jax.ShapeDtypeStruct((group_count * rows, coarse_depth), jnp.float32)

    def stage(count):
        return pltpu.VMEM((count, fields, pieces, cells_across, 128), jnp.float32)

    if box_count == 2:
        other = lax.ppermute(current, "box", [(0, 1), (1, 0)])
        copies = (cells_along + 2) * pieces + 2
        shapes = [
            current.shape,
            (2, 3 * fields, 2, half_across, cells_depth),
            (fields, half_across, cells_depth),
            (cells_along // 2 - 1, fields, half_across, cells_depth),
            (capacity * group_count, total),
            (capacity * group_count, coarse_depth),
        ]
        early, carry, face, sums, selection, codes = pl.pallas_call(
            functools.partial(early_kernel, group_count, capacity),
            out_shape=[pltpu.VMEM(shape, jnp.float32) for shape in shapes],
            in_specs=[hbm] * 4,
            out_specs=[vmem] * len(shapes),
            scratch_shapes=[
                stage(2 * cells_along),
                pltpu.VMEM((1, total), jnp.int32),
                pltpu.VMEM((1, total), jnp.int32),
                pltpu.SemaphoreType.DMA((copies,)),
            ],
            compiler_params=params,
            cost_estimate=pl.CostEstimate(
                flops=200 * current.size, bytes_accessed=8 * current.size, transcendentals=0
            ),
            name="early",
        )(*(
            pltpu.with_memory_space_constraint(values, pltpu.HBM)
            for values in (fine_state, patch_ghosts, dest_grp[0], dest_column[0])
        ))
        updated, outgoing = pl.pallas_call(
            functools.partial(late_kernel, group_count, capacity, rows),
            out_shape=[
                pltpu.VMEM(current.shape, jnp.float32),
                pltpu.VMEM(outgoing_shape.shape, jnp.float32),
            ],
            in_specs=[vmem] * 7,
            out_specs=[vmem] * 2,
            scratch_shapes=[stage(4)],
            input_output_aliases={6: 0},
            compiler_params=params,
            name="late",
        )(carry, other, face, sums, selection, codes, early)
    else:
        ends = box_count - 1
        low = lax.ppermute(current[:, -2:], "box", [(i, i + 1) for i in range(ends)])
        high = lax.ppermute(current[:, :2], "box", [(i + 1, i) for i in range(ends)])
        updated, outgoing = pl.pallas_call(
            functools.partial(patch_kernel, box_count, group_count, capacity, rows),
            out_shape=[jax.ShapeDtypeStruct(current.shape, jnp.float32), outgoing_shape],
            in_specs=[vmem] * 6,
            out_specs=[vmem] * 2,
            scratch_shapes=[
                pltpu.VMEM((cells_along + 2, fields, 2, half_across, cells_depth), jnp.float32),
                stage(2 * cells_along + 8),
            ],
            compiler_params=params,
            name="patch",
        )(current, patch_ghosts[0], low, high, dest_grp[0], dest_column[0])
    incoming = lax.all_to_all(
        outgoing.reshape(group_count, rows, coarse_depth),
        "grp", split_axis=0, concat_axis=0, tiled=True,
    ).reshape(group_count * rows, coarse_depth)
    coarse_new, final = pl.pallas_call(
        functools.partial(owner_kernel, group_count, capacity, rows),
        out_shape=[
            jax.ShapeDtypeStruct((fields, total, coarse_depth), jnp.float32),
            jax.ShapeDtypeStruct(current.shape, jnp.float32),
        ],
        in_specs=[vmem] * 4,
        out_specs=[hbm, hbm],
        scratch_shapes=[
            pltpu.VMEM((fields, total, coarse_depth), jnp.float32),
            pltpu.SemaphoreType.DMA((2,)),
        ],
        compiler_params=params,
        name="owner",
    )(
        incoming,
        coarse_state[0, 0].transpose(1, 0, 2),
        coarse_face_term[0, 0].transpose(1, 0, 2),
        pltpu.with_memory_space_constraint(updated, pltpu.VMEM),
    )
    return (final[None], coarse_new.transpose(1, 0, 2)[None, None])


def solution(mesh):
    in_specs = (
        P("grp", None, "box", None, None),
        P("grp", None, None, None, None, None),
        P("grp", "box", None, None, None),
        P("grp", "box", None, None, None),
        P("grp", "box", None),
        P("grp", "box", None),
    )
    out_specs = (P("grp", None, "box", None, None), P("grp", "box", None, None, None))
    return jax.shard_map(
        on_device, mesh=mesh, in_specs=in_specs, out_specs=out_specs, check_vma=False
    )
```

```python
import functools
import math

import jax
import jax.numpy as jnp
from jax import lax
from jax.experimental import pallas as pl
from jax.experimental.pallas import tpu as pltpu
from jax.sharding import PartitionSpec as P

gamma_ratio = 1.4
time_step = 0.06
vmem_limit = 8 * 1024 * 1024


def split_dot(lhs, rhs, split_lhs, dims=(((1,), (0,)), ((), ()))):
    data = lhs if split_lhs else rhs
    exact = (rhs if split_lhs else lhs).astype(jnp.bfloat16)
    total = None
    for _ in range(3):
        term = data.astype(jnp.bfloat16)
        data = data - term.astype(jnp.float32)
        pair = (term, exact) if split_lhs else (exact, term)
        part = lax.dot_general(*pair, dims, preferred_element_type=jnp.float32)
        total = part if total is None else total + part
    return total


def next_z(values):
    return pltpu.roll(values, values.shape[-1] - 1, 1)


def last_z(values):
    return pltpu.roll(values, 1, 1)


def next_y(pair):
    even, odd = pair
    return (odd, pltpu.roll(even, even.shape[0] - 1, 0))


def last_y(pair):
    even, odd = pair
    return (pltpu.roll(odd, 1, 0), even)


def both(function, *pairs):
    return tuple(function(*halves) for halves in zip(*pairs))


class Cells:

    def __init__(self, state):
        density, mom = state[0], state[1:4]
        inverse = both(lambda d: 1.0 / d, density)
        velocity = [both(lambda m, r: m * r, m, inverse) for m in mom]
        square = {}
        for i in range(3):
            for j in range(i, 3):
                square[i, j] = both(lambda m, v: m * v, mom[i], velocity[j])
        pressure = both(
            lambda e, a, b, c: (gamma_ratio - 1.0) * (e - 0.5 * (a + b + c)),
            state[4], square[0, 0], square[1, 1], square[2, 2],
        )
        square_sound = both(lambda p, r: gamma_ratio * p * r, pressure, inverse)
        sound = both(lambda q: q * lax.rsqrt(q), square_sound)
        enthalpy = both(jnp.add, state[4], pressure)
        self.state = state
        self.flux = []
        self.speed = []
        for normal in range(3):
            pieces = [mom[normal]]
            for member in range(3):
                term = square[min(member, normal), max(member, normal)]
                pieces.append(both(jnp.add, term, pressure) if member == normal else term)
            pieces.append(both(jnp.multiply, enthalpy, velocity[normal]))
            self.flux.append(pieces)
            self.speed.append(both(lambda v, c: jnp.abs(v) + c, velocity[normal], sound))


def doubled_face(left_state, right_state, left_flux, right_flux, left_speed, right_speed):
    biggest = both(jnp.maximum, left_speed, right_speed)
    return [
        both(lambda a, b, f, g, s: (f + g) - s * (b - a), ls, rs, lf, rf, biggest)
        for ls, rs, lf, rf in zip(left_state, right_state, left_flux, right_flux)
    ]


def x_face(left, right):
    return doubled_face(
        left.state, right.state, left.flux[0], right.flux[0], left.speed[0], right.speed[0]
    )


def side_change(cells):
    change = [None] * len(cells.state)
    for normal in (1, 2):
        if normal == 1:
            ahead, behind = next_y, last_y
        else:
            ahead = functools.partial(both, next_z)
            behind = functools.partial(both, last_z)
        faces = doubled_face(
            cells.state, [ahead(s) for s in cells.state],
            cells.flux[normal], [ahead(f) for f in cells.flux[normal]],
            cells.speed[normal], ahead(cells.speed[normal]),
        )
        for index, face in enumerate(faces):
            part = both(jnp.subtract, face, behind(face))
            change[index] = part if change[index] is None else both(jnp.add, change[index], part)
    return change


def advance(layers, on_update, on_face):
    before, low_face, change = Cells(layers[0]()), None, None
    for index in range(1, len(layers)):
        here = Cells(layers[index]())
        face = x_face(before, here)
        on_face(index - 1, face)
        if index >= 2:
            half = 0.5 * time_step
            on_update(
                index - 1,
                [
                    both(lambda u, c, h, l: u - half * (c + (h - l)), u, c, h, l)
                    for u, c, h, l in zip(before.state, change, face, low_face)
                ],
            )
        if index < len(layers) - 1:
            change = side_change(here)
        before, low_face = here, face


def step_state(state, change, high_face, low_face):
    half = 0.5 * time_step
    return [
        both(lambda u, c, h, l: u - half * (c + (h - l)), u, c, h, l)
        for u, c, h, l in zip(state, change, high_face, low_face)
    ]


def split_z(ref, slot, field, half_across):
    return tuple(
        jnp.concatenate(
            [
                ref[slot, field, piece, pl.ds(parity, half_across, stride=2), :]
                for piece in range(ref.shape[2])
            ],
            axis=1,
        )
        for parity in (0, 1)
    )


def put_layer(stage_ref, slot, new_ref, layer, state, turn):
    fields, pieces, _, lanes = stage_ref.shape[1:]
    half_across = state[0][0].shape[0]
    for f in range(fields):
        for piece in range(pieces):
            part = slice(piece * lanes, (piece + 1) * lanes)
            for parity in (0, 1):
                values = state[f][parity][:, part]
                stage_ref[slot, f, piece, pl.ds(parity, half_across, stride=2), :] = (
                    turn * values if f == 1 else values
                )
            new_ref[f, layer, :, part] = stage_ref[slot, f, piece]


class Carried:

    def __init__(self, ref, slot, fields):
        def pair(index):
            return tuple(ref[slot, index, parity] for parity in (0, 1))

        self.state = [pair(f) for f in range(fields)]
        self.flux = [[self.state[1]] + [pair(fields + f) for f in range(1, fields)]]
        self.speed = [pair(fields)]
        self.partial = [pair(2 * fields + f) for f in range(fields)]

    @staticmethod
    def keep(ref, slot, cells, change, low_face):
        half = 0.5 * time_step
        fields = len(cells.state)
        for f in range(fields):
            for parity in (0, 1):
                ref[slot, f, parity] = cells.state[f][parity]
                ref[slot, 2 * fields + f, parity] = cells.state[f][parity] - half * (
                    change[f][parity] - low_face[f][parity]
                )
                ref[slot, fields + f, parity] = (
                    cells.flux[0][f][parity] if f > 0 else cells.speed[0][parity]
                )

    def finished(self, high_face):
        half = 0.5 * time_step
        return [both(lambda p, h: p - half * h, p, h) for p, h in zip(self.partial, high_face)]


def early_kernel(
    groups, capacity, fine_ref, ghost_ref, owner_ref, column_ref, state_ref, term_ref,
    new_ref, carry_ref, face_ref, sum_ref, select_ref, code_ref, state_vmem, term_vmem,
    stage_ref, owner_vmem, column_vmem, copy_sems,
):
    _, fields, along, across, depth = fine_ref.shape
    half_across = across // 2
    lanes = stage_ref.shape[-1]
    pieces = depth // lanes
    at_high = lax.axis_index("box") == 1
    side = jnp.where(at_high, 1, 0)
    turn = jnp.where(at_high, -1.0, 1.0)

    copies = {}

    def fetch(slot, source):
        for piece in range(pieces):
            copies[slot, piece] = pltpu.make_async_copy(
                source(slice(piece * lanes, (piece + 1) * lanes)),
                stage_ref.at[slot, :, piece],
                copy_sems.at[slot * pieces + piece],
            )
            copies[slot, piece].start()

    ghost_slots = (0, along + 1)
    fetch(0, lambda part: ghost_ref.at[0, 0, side, :, :, part])
    for index in range(along):
        layer = jnp.where(at_high, along - 1 - index, index)
        fetch(1 + index, lambda part, layer=layer: fine_ref.at[0, :, layer, :, part])
    fetch(along + 1, lambda part: ghost_ref.at[0, 1, side, :, :, part])
    pairs = (
        (owner_ref, owner_vmem), (column_ref, column_vmem),
        (state_ref, state_vmem), (term_ref, term_vmem),
    )
    small = [
        pltpu.make_async_copy(source, target, copy_sems.at[(along + 2) * pieces + index])
        for index, (source, target) in enumerate(pairs)
    ]
    for copy in small:
        copy.start()

    def arrived(slot):
        if slot in (0, 3):
            for (at, _), copy in copies.items():
                if (at < 3) == (slot == 0):
                    copy.wait()
        planes = [split_z(stage_ref, slot, f, half_across) for f in range(fields)]
        planes[1] = tuple(turn * values for values in planes[1])
        return planes

    ghost_now = arrived(0)
    before, low_face, change = Cells(ghost_now), None, None
    faces = []
    halves = []
    for index in range(along):
        here = Cells(arrived(1 + index))
        face = x_face(before, here)
        if index == 0:
            faces.append(face)
        else:
            halves.append(step_state(before.state, change, face, low_face))
        change = side_change(here)
        before, low_face = here, face
    Carried.keep(carry_ref, 0, before, change, low_face)

    ghost_end = arrived(along + 1)
    before = Cells(
        [both(lambda a, b: 0.5 * a + 0.5 * b, a, b) for a, b in zip(ghost_now, ghost_end)]
    )
    low_face, change = None, None
    total_sums = {}
    for index in range(along - 1):
        here = Cells(halves[index])
        face = x_face(before, here)
        if index == 0:
            faces.append(face)
        else:
            state = step_state(before.state, change, face, low_face)
            layer = jnp.where(at_high, along - index, index - 1)
            put_layer(stage_ref, along + 1 + index, new_ref, layer, state, turn)
            for f in range(fields):
                key = (index - 1) // 2, f
                pooled = state[f][0] + state[f][1]
                total_sums[key] = total_sums[key] + pooled if key in total_sums else pooled
        change = side_change(here)
        before, low_face = here, face
    Carried.keep(carry_ref, 1, before, change, low_face)
    for (plane, f), pooled in total_sums.items():
        sum_ref[plane, f] = pooled
    for f in range(fields):
        both_steps = [faces[0][f][parity] + faces[1][f][parity] for parity in (0, 1)]
        face_ref[f] = both_steps[0] + both_steps[1]

    for copy in small:
        copy.wait()
    total = owner_vmem.shape[1]
    count_average = (along // 2) * half_across
    selections = one_hot_slots(owner_vmem[...], groups, capacity)
    record_ids = lax.broadcasted_iota(jnp.int32, (1, total), 1)
    codes = (column_vmem[...] + 1).astype(jnp.float32)
    codes = jnp.where(record_ids < count_average, codes, -codes)
    for slot in range(capacity):
        rows = slice(slot * groups, (slot + 1) * groups)
        select_ref[rows] = selections[slot]
        code = jnp.sum(selections[slot] * codes, axis=1, keepdims=True)
        code_ref[rows] = jnp.broadcast_to(code, (groups, code_ref.shape[1]))


def late_kernel(
    groups, capacity, rows, carry_ref, other_ref, face_ref, sum_ref, select_ref, code_ref,
    early_ref, new_ref, out_ref, stage_ref,
):
    del early_ref
    fields, along, across, depth = other_ref.shape
    half_across = across // 2
    lanes = stage_ref.shape[-1]
    pieces = depth // lanes
    at_high = lax.axis_index("box") == 1
    turn = jnp.where(at_high, -1.0, 1.0)

    def place(index):
        return jnp.where(at_high, along - 1 - index, index)

    def received(index):
        for f in range(fields):
            plane = other_ref[f, place(index)]
            for piece in range(pieces):
                stage_ref[index, f, piece] = plane[:, piece * lanes:(piece + 1) * lanes]
        planes = [split_z(stage_ref, index, f, half_across) for f in range(fields)]
        planes[1] = tuple(turn * values for values in planes[1])
        return planes

    near = Cells(received(0))
    end = Carried(carry_ref, 0, fields)
    end_face = x_face(end, near)
    end_half = end.finished(end_face)
    near_half = step_state(
        near.state, side_change(near), x_face(near, Cells(received(1))), end_face
    )
    inner = Carried(carry_ref, 1, fields)
    last = Cells(end_half)
    inner_face = x_face(inner, last)
    inner_new = inner.finished(inner_face)
    last_new = step_state(
        last.state, side_change(last), x_face(last, Cells(near_half)), inner_face
    )
    put_layer(stage_ref, 2, new_ref, place(along - 2), inner_new, turn)
    put_layer(stage_ref, 3, new_ref, place(along - 1), last_new, turn)

    planes = along // 2
    blocks = []
    for f in range(fields):
        sums = [sum_ref[plane, f] for plane in range(planes - 1)]
        sums.append(
            (inner_new[f][0] + inner_new[f][1]) + (last_new[f][0] + last_new[f][1])
        )
        scale = turn if f == 1 else 1.0
        for plane in range(planes):
            blocks.append(
                (0.125 * scale) * jnp.where(at_high, sums[planes - 1 - plane], sums[plane])
            )
        blocks.append((-0.5 * time_step / 8 * scale) * face_ref[f])
    route(
        jnp.concatenate(blocks, axis=0), select_ref[...], groups, capacity, rows, fields, out_ref
    )
    for slot in range(capacity):
        out_ref[pl.ds(slot * (fields + 1) + fields, groups, stride=rows), :] = code_ref[
            slot * groups:(slot + 1) * groups
        ]


def route(stacked, selection, groups, capacity, rows, fields, out_ref):
    depth, coarse_depth = stacked.shape[1], out_ref.shape[1]
    lane_pair = lax.broadcasted_iota(jnp.int32, (depth, coarse_depth), 0) // 2
    pool = jnp.where(
        lane_pair == lax.broadcasted_iota(jnp.int32, (depth, coarse_depth), 1), 1.0, 0.0
    )
    records = split_dot(stacked, pool, True)
    total = records.shape[0] // fields
    wide = jnp.concatenate(
        [records[f * total:(f + 1) * total] for f in range(fields)], axis=1
    )
    chosen = split_dot(selection, wide, False)
    for slot in range(capacity):
        for f in range(fields):
            out_ref[pl.ds(slot * (fields + 1) + f, groups, stride=rows), :] = chosen[
                slot * groups:(slot + 1) * groups, f * coarse_depth:(f + 1) * coarse_depth
            ]


def one_hot_slots(owners, groups, capacity):
    total = owners.shape[1]
    hit = owners == lax.broadcasted_iota(jnp.int32, (groups, total), 0)
    hot = jnp.where(hit, 1.0, 0.0)
    earlier = (
        lax.broadcasted_iota(jnp.int32, (total, total), 0)
        < lax.broadcasted_iota(jnp.int32, (total, total), 1)
    )
    rank = jnp.dot(
        hot.astype(jnp.bfloat16),
        jnp.where(earlier, 1.0, 0.0).astype(jnp.bfloat16),
        preferred_element_type=jnp.float32,
    )
    return [jnp.where(hit & (rank == float(slot)), 1.0, 0.0) for slot in range(capacity)]


def patch_kernel(
    box_count, groups, capacity, rows,
    fine_ref, ghost_ref, low_ref, high_ref, owner_ref, column_ref,
    new_ref, out_ref, half_ref, stage_ref,
):
    box_place = lax.axis_index("box")
    at_low = box_place == 0
    at_high = box_place == box_count - 1
    fields, along, across, depth = fine_ref.shape
    half_across = across // 2
    lanes = stage_ref.shape[-1]
    pieces = depth // lanes
    slots = iter(range(stage_ref.shape[0]))

    def parted(planes):
        slot = next(slots)
        for f, plane in enumerate(planes):
            for piece in range(pieces):
                stage_ref[slot, f, piece] = plane[:, piece * lanes:(piece + 1) * lanes]
        return [split_z(stage_ref, slot, f, half_across) for f in range(fields)]

    def rows_of(ref, layer):
        return parted([ref[f, layer] for f in range(fields)])

    def ghost_layer(at, time_frac):
        return parted(
            [
                (1.0 - time_frac) * ghost_ref[0, at, f] + time_frac * ghost_ref[1, at, f]
                for f in range(fields)
            ]
        )

    def half_layer(index):
        return [tuple(half_ref[index, f, parity] for parity in (0, 1)) for f in range(fields)]

    def picked(flag, first, second):
        return [both(lambda a, b: jnp.where(flag, a, b), a, b) for a, b in zip(first, second)]

    width = low_ref.shape[1]
    first = [lambda: rows_of(low_ref, width - 2)]
    first += [lambda: picked(at_low, ghost_layer(0, 0.0), rows_of(low_ref, width - 1))]
    first += [functools.partial(rows_of, fine_ref, index) for index in range(along)]
    first += [lambda: picked(at_high, ghost_layer(1, 0.0), rows_of(high_ref, 0))]
    first += [lambda: rows_of(high_ref, 1)]
    second = [lambda: picked(at_low, ghost_layer(0, 0.5), half_layer(0))]
    second += [functools.partial(half_layer, 1 + index) for index in range(along)]
    second += [lambda: picked(at_high, ghost_layer(1, 0.5), half_layer(along + 1))]
    low_at, high_at = (1, 0), (along + 1, along)
    low_faces, high_faces, sums = [], [], {}

    def keep_half(index, state):
        for f in range(fields):
            for parity in (0, 1):
                half_ref[index - 1, f, parity] = state[f][parity]

    def keep_new(index, state):
        put_layer(stage_ref, next(slots), new_ref, index - 1, state, 1.0)
        for f in range(fields):
            pooled = state[f][0] + state[f][1]
            key = (f, (index - 1) // 2)
            sums[key] = sums[key] + pooled if key in sums else pooled

    def face_keeper(step):
        def keep(index, face):
            if index == low_at[step]:
                low_faces.append(face)
            if index == high_at[step]:
                high_faces.append(face)
        return keep

    advance(first, keep_half, face_keeper(0))
    advance(second, keep_new, face_keeper(1))

    planes = along // 2
    blocks = []
    for f in range(fields):
        blocks += [0.125 * sums[f, plane] for plane in range(planes)]
        low = [low_faces[0][f][parity] + low_faces[1][f][parity] for parity in (0, 1)]
        high = [high_faces[0][f][parity] + high_faces[1][f][parity] for parity in (0, 1)]
        face_sum = jnp.where(at_low, low[0] + low[1], -(high[0] + high[1]))
        blocks.append((-0.5 * time_step / 8) * face_sum)
    total = owner_ref.shape[1]
    selections = one_hot_slots(owner_ref[...], groups, capacity)
    route(
        jnp.concatenate(blocks, axis=0), jnp.concatenate(selections, axis=0),
        groups, capacity, rows, fields, out_ref,
    )
    record_ids = lax.broadcasted_iota(jnp.int32, (1, total), 1)
    codes = (column_ref[...] + 1).astype(jnp.float32)
    face_code = jnp.where(at_low | at_high, -codes, 0.0)
    codes = jnp.where(record_ids < planes * half_across, codes, face_code)
    for slot in range(capacity):
        code = jnp.sum(selections[slot] * codes, axis=1, keepdims=True)
        out_ref[pl.ds(slot * (fields + 1) + fields, groups, stride=rows), :] = jnp.broadcast_to(
            code, (groups, out_ref.shape[1])
        )


def owner_kernel(
    groups, capacity, rows, in_ref, state_ref, term_ref, new_ref,
    coarse_ref, final_ref, out_ref, copy_sems,
):
    write_fine = pltpu.make_async_copy(new_ref, final_ref, copy_sems.at[0])
    write_fine.start()
    fields, total, coarse_depth = state_ref.shape
    codes, values = [], []
    for slot in range(capacity):
        base = slot * (fields + 1)
        code = in_ref[pl.ds(base + fields, groups, stride=rows), :]
        codes.append(code)
        values.append(
            jnp.concatenate(
                [
                    jnp.where(code != 0.0, in_ref[pl.ds(base + f, groups, stride=rows), :], 0.0)
                    for f in range(fields)
                ],
                axis=1,
            )
        )
    codes = jnp.concatenate(codes, axis=0)
    values = jnp.concatenate(values, axis=0)
    count = codes.shape[0]
    across = jnp.transpose(codes)[:total]
    column = (lax.broadcasted_iota(jnp.int32, (total, count), 0) + 1).astype(jnp.float32)
    hot = jnp.where(jnp.abs(across) == column, 1.0, 0.0)
    kind = jnp.where(codes > 0.0, 1.0, jnp.where(codes < 0.0, -1.0, 0.0))
    flag = jnp.dot(
        hot.astype(jnp.bfloat16), kind.astype(jnp.bfloat16), preferred_element_type=jnp.float32
    )
    got = split_dot(hot, values, False)
    for f in range(fields):
        value = got[:, f * coarse_depth:(f + 1) * coarse_depth]
        state = state_ref[f]
        refluxed = state + (value - term_ref[f])
        out_ref[f] = jnp.where(flag > 0.0, value, jnp.where(flag < 0.0, refluxed, state))
    write_coarse = pltpu.make_async_copy(out_ref, coarse_ref, copy_sems.at[1])
    write_coarse.start()
    write_fine.wait()
    write_coarse.wait()


def on_device(fine_state, patch_ghosts, coarse_state, coarse_face_term, dest_grp, dest_column):
    box_count = lax.axis_size("box")
    group_count = lax.axis_size("grp")
    current = fine_state[0]
    fields, cells_along, cells_across, cells_depth = current.shape
    total = dest_grp.shape[-1]
    capacity = (total + group_count - 1) // group_count
    rows = capacity * (fields + 1)
    inner_rows = math.gcd(rows, 8)
    coarse_depth = cells_depth // 2
    owned_state = coarse_state[0, 0].transpose(1, 0, 2)
    owned_term = coarse_face_term[0, 0].transpose(1, 0, 2)
    params = pltpu.CompilerParams(vmem_limit_bytes=vmem_limit)
    vmem = pl.BlockSpec(memory_space=pltpu.VMEM)
    hbm = pl.BlockSpec(memory_space=pltpu.HBM)
    half_across, pieces = cells_across // 2, cells_depth // 128
    outgoing_shape = jax.ShapeDtypeStruct((group_count * rows, coarse_depth), jnp.float32)

    def stage(count):
        return pltpu.VMEM((count, fields, pieces, cells_across, 128), jnp.float32)

    if box_count == 2:
        other = lax.ppermute(current, "box", [(0, 1), (1, 0)])
        copies = (cells_along + 2) * pieces + 4
        shapes = [
            current.shape,
            (2, 3 * fields, 2, half_across, cells_depth),
            (fields, half_across, cells_depth),
            (cells_along // 2 - 1, fields, half_across, cells_depth),
            (capacity * group_count, total),
            (capacity * group_count, coarse_depth),
            owned_state.shape,
            owned_term.shape,
        ]
        early, carry, face, sums, selection, codes, owned_state, owned_term = pl.pallas_call(
            functools.partial(early_kernel, group_count, capacity),
            out_shape=[pltpu.VMEM(shape, jnp.float32) for shape in shapes],
            in_specs=[hbm] * 6,
            out_specs=[vmem] * len(shapes),
            scratch_shapes=[
                stage(2 * cells_along),
                pltpu.VMEM((1, total), jnp.int32),
                pltpu.VMEM((1, total), jnp.int32),
                pltpu.SemaphoreType.DMA((copies,)),
            ],
            compiler_params=params,
            cost_estimate=pl.CostEstimate(
                flops=200 * current.size, bytes_accessed=8 * current.size, transcendentals=0
            ),
            name="early",
        )(*(
            pltpu.with_memory_space_constraint(values, pltpu.HBM)
            for values in (
                fine_state, patch_ghosts, dest_grp[0], dest_column[0], owned_state, owned_term
            )
        ))
        updated, outgoing = pl.pallas_call(
            functools.partial(late_kernel, group_count, capacity, rows),
            out_shape=[
                pltpu.VMEM(current.shape, jnp.float32),
                pltpu.VMEM(outgoing_shape.shape, jnp.float32),
            ],
            in_specs=[vmem] * 7,
            out_specs=[vmem] * 2,
            scratch_shapes=[stage(4)],
            input_output_aliases={6: 0},
            compiler_params=params,
            name="late",
        )(carry, other, face, sums, selection, codes, early)
    else:
        ends = box_count - 1
        low = lax.ppermute(current[:, -2:], "box", [(i, i + 1) for i in range(ends)])
        high = lax.ppermute(current[:, :2], "box", [(i + 1, i) for i in range(ends)])
        updated, outgoing = pl.pallas_call(
            functools.partial(patch_kernel, box_count, group_count, capacity, rows),
            out_shape=[jax.ShapeDtypeStruct(current.shape, jnp.float32), outgoing_shape],
            in_specs=[vmem] * 6,
            out_specs=[vmem] * 2,
            scratch_shapes=[
                pltpu.VMEM((cells_along + 2, fields, 2, half_across, cells_depth), jnp.float32),
                stage(2 * cells_along + 8),
            ],
            compiler_params=params,
            name="patch",
        )(current, patch_ghosts[0], low, high, dest_grp[0], dest_column[0])
    incoming = lax.all_to_all(
        outgoing.reshape(group_count, rows // inner_rows, inner_rows, coarse_depth),
        "grp", split_axis=0, concat_axis=0, tiled=True,
    ).reshape(group_count * rows, coarse_depth)
    coarse_new, final = pl.pallas_call(
        functools.partial(owner_kernel, group_count, capacity, rows),
        out_shape=[
            jax.ShapeDtypeStruct((fields, total, coarse_depth), jnp.float32),
            jax.ShapeDtypeStruct(current.shape, jnp.float32),
        ],
        in_specs=[vmem] * 4,
        out_specs=[hbm, hbm],
        scratch_shapes=[
            pltpu.VMEM((fields, total, coarse_depth), jnp.float32),
            pltpu.SemaphoreType.DMA((2,)),
        ],
        compiler_params=params,
        name="owner",
    )(
        incoming,
        pltpu.with_memory_space_constraint(owned_state, pltpu.VMEM),
        pltpu.with_memory_space_constraint(owned_term, pltpu.VMEM),
        pltpu.with_memory_space_constraint(updated, pltpu.VMEM),
    )
    return (final[None], coarse_new.transpose(1, 0, 2)[None, None])


def solution(mesh):
    in_specs = (
        P("grp", None, "box", None, None),
        P("grp", None, None, None, None, None),
        P("grp", "box", None, None, None),
        P("grp", "box", None, None, None),
        P("grp", "box", None),
        P("grp", "box", None),
    )
    out_specs = (P("grp", None, "box", None, None), P("grp", "box", None, None, None))
    return jax.shard_map(
        on_device, mesh=mesh, in_specs=in_specs, out_specs=out_specs, check_vma=False
    )
```

```python
import functools
import math

import jax
import jax.numpy as jnp
from jax import lax
from jax.experimental import pallas as pl
from jax.experimental.pallas import tpu as pltpu
from jax.sharding import PartitionSpec as P

gamma_ratio = 1.4
time_step = 0.06
vmem_limit = 8 * 1024 * 1024


def split_dot(lhs, rhs, split_lhs, dims=(((1,), (0,)), ((), ()))):
    data = lhs if split_lhs else rhs
    exact = (rhs if split_lhs else lhs).astype(jnp.bfloat16)
    total = None
    for _ in range(3):
        term = data.astype(jnp.bfloat16)
        data = data - term.astype(jnp.float32)
        pair = (term, exact) if split_lhs else (exact, term)
        part = lax.dot_general(*pair, dims, preferred_element_type=jnp.float32)
        total = part if total is None else total + part
    return total


def next_z(values):
    return pltpu.roll(values, values.shape[-1] - 1, 1)


def last_z(values):
    return pltpu.roll(values, 1, 1)


def next_y(pair):
    even, odd = pair
    return (odd, pltpu.roll(even, even.shape[0] - 1, 0))


def last_y(pair):
    even, odd = pair
    return (pltpu.roll(odd, 1, 0), even)


def both(function, *pairs):
    return tuple(function(*halves) for halves in zip(*pairs))


class Cells:

    def __init__(self, state):
        density, mom = state[0], state[1:4]
        inverse = both(lambda d: 1.0 / d, density)
        velocity = [both(lambda m, r: m * r, m, inverse) for m in mom]
        square = {}
        for i in range(3):
            for j in range(i, 3):
                square[i, j] = both(lambda m, v: m * v, mom[i], velocity[j])
        pressure = both(
            lambda e, a, b, c: (gamma_ratio - 1.0) * (e - 0.5 * (a + b + c)),
            state[4], square[0, 0], square[1, 1], square[2, 2],
        )
        square_sound = both(lambda p, r: gamma_ratio * p * r, pressure, inverse)
        sound = both(lambda q: q * lax.rsqrt(q), square_sound)
        enthalpy = both(jnp.add, state[4], pressure)
        self.state = state
        self.flux = []
        self.speed = []
        for normal in range(3):
            pieces = [mom[normal]]
            for member in range(3):
                term = square[min(member, normal), max(member, normal)]
                pieces.append(both(jnp.add, term, pressure) if member == normal else term)
            pieces.append(both(jnp.multiply, enthalpy, velocity[normal]))
            self.flux.append(pieces)
            self.speed.append(both(lambda v, c: jnp.abs(v) + c, velocity[normal], sound))


def doubled_face(left_state, right_state, left_flux, right_flux, left_speed, right_speed):
    biggest = both(jnp.maximum, left_speed, right_speed)
    return [
        both(lambda a, b, f, g, s: (f + g) - s * (b - a), ls, rs, lf, rf, biggest)
        for ls, rs, lf, rf in zip(left_state, right_state, left_flux, right_flux)
    ]


def x_face(left, right):
    return doubled_face(
        left.state, right.state, left.flux[0], right.flux[0], left.speed[0], right.speed[0]
    )


def side_change(cells):
    change = [None] * len(cells.state)
    for normal in (1, 2):
        if normal == 1:
            ahead, behind = next_y, last_y
        else:
            ahead = functools.partial(both, next_z)
            behind = functools.partial(both, last_z)
        faces = doubled_face(
            cells.state, [ahead(s) for s in cells.state],
            cells.flux[normal], [ahead(f) for f in cells.flux[normal]],
            cells.speed[normal], ahead(cells.speed[normal]),
        )
        for index, face in enumerate(faces):
            part = both(jnp.subtract, face, behind(face))
            change[index] = part if change[index] is None else both(jnp.add, change[index], part)
    return change


def advance(layers, on_update, on_face):
    before, low_face, change = Cells(layers[0]()), None, None
    for index in range(1, len(layers)):
        here = Cells(layers[index]())
        face = x_face(before, here)
        on_face(index - 1, face)
        if index >= 2:
            half = 0.5 * time_step
            on_update(
                index - 1,
                [
                    both(lambda u, c, h, l: u - half * (c + (h - l)), u, c, h, l)
                    for u, c, h, l in zip(before.state, change, face, low_face)
                ],
            )
        if index < len(layers) - 1:
            change = side_change(here)
        before, low_face = here, face


def step_state(state, change, high_face, low_face):
    half = 0.5 * time_step
    return [
        both(lambda u, c, h, l: u - half * (c + (h - l)), u, c, h, l)
        for u, c, h, l in zip(state, change, high_face, low_face)
    ]


def split_z(ref, slot, field, half_across):
    return tuple(
        jnp.concatenate(
            [
                ref[slot, field, piece, pl.ds(parity, half_across, stride=2), :]
                for piece in range(ref.shape[2])
            ],
            axis=1,
        )
        for parity in (0, 1)
    )


def put_layer(stage_ref, slot, new_ref, layer, state, turn):
    fields, pieces, _, lanes = stage_ref.shape[1:]
    half_across = state[0][0].shape[0]
    for f in range(fields):
        for piece in range(pieces):
            part = slice(piece * lanes, (piece + 1) * lanes)
            for parity in (0, 1):
                values = state[f][parity][:, part]
                stage_ref[slot, f, piece, pl.ds(parity, half_across, stride=2), :] = (
                    turn * values if f == 1 else values
                )
            new_ref[f, layer, :, part] = stage_ref[slot, f, piece]


class Carried:

    def __init__(self, ref, slot, fields):
        def pair(index):
            return tuple(ref[slot, index, parity] for parity in (0, 1))

        self.state = [pair(f) for f in range(fields)]
        self.flux = [[self.state[1]] + [pair(fields + f) for f in range(1, fields)]]
        self.speed = [pair(fields)]
        self.partial = [pair(2 * fields + f) for f in range(fields)]

    @staticmethod
    def keep(ref, slot, cells, change, low_face):
        half = 0.5 * time_step
        fields = len(cells.state)
        for f in range(fields):
            for parity in (0, 1):
                ref[slot, f, parity] = cells.state[f][parity]
                ref[slot, 2 * fields + f, parity] = cells.state[f][parity] - half * (
                    change[f][parity] - low_face[f][parity]
                )
                ref[slot, fields + f, parity] = (
                    cells.flux[0][f][parity] if f > 0 else cells.speed[0][parity]
                )

    def finished(self, high_face):
        half = 0.5 * time_step
        return [both(lambda p, h: p - half * h, p, h) for p, h in zip(self.partial, high_face)]


def early_kernel(
    groups, capacity, fine_ref, ghost_ref, owner_ref, column_ref, state_ref, term_ref,
    new_ref, carry_ref, face_ref, sum_ref, select_ref, code_ref, state_vmem, term_vmem,
    stage_ref, owner_vmem, column_vmem, copy_sems,
):
    _, fields, along, across, depth = fine_ref.shape
    half_across = across // 2
    lanes = stage_ref.shape[-1]
    pieces = depth // lanes
    at_high = lax.axis_index("box") == 1
    side = jnp.where(at_high, 1, 0)
    turn = jnp.where(at_high, -1.0, 1.0)

    copies = {}

    def fetch(slot, source):
        for piece in range(pieces):
            copies[slot, piece] = pltpu.make_async_copy(
                source(slice(piece * lanes, (piece + 1) * lanes)),
                stage_ref.at[slot, :, piece],
                copy_sems.at[slot * pieces + piece],
            )
            copies[slot, piece].start()

    ghost_slots = (0, along + 1)
    fetch(0, lambda part: ghost_ref.at[0, 0, side, :, :, part])
    for index in range(along):
        layer = jnp.where(at_high, along - 1 - index, index)
        fetch(1 + index, lambda part, layer=layer: fine_ref.at[0, :, layer, :, part])
    fetch(along + 1, lambda part: ghost_ref.at[0, 1, side, :, :, part])
    pairs = (
        (owner_ref, owner_vmem), (column_ref, column_vmem),
        (state_ref, state_vmem), (term_ref, term_vmem),
    )
    small = [
        pltpu.make_async_copy(source, target, copy_sems.at[(along + 2) * pieces + index])
        for index, (source, target) in enumerate(pairs)
    ]
    for copy in small:
        copy.start()

    def arrived(slot):
        if slot in (0, 3):
            for (at, _), copy in copies.items():
                if (at < 3) == (slot == 0):
                    copy.wait()
        planes = [split_z(stage_ref, slot, f, half_across) for f in range(fields)]
        planes[1] = tuple(turn * values for values in planes[1])
        return planes

    ghost_now = arrived(0)
    before, low_face, change = Cells(ghost_now), None, None
    faces = []
    halves = []
    for index in range(along):
        here = Cells(arrived(1 + index))
        face = x_face(before, here)
        if index == 0:
            faces.append(face)
        else:
            halves.append(step_state(before.state, change, face, low_face))
        change = side_change(here)
        before, low_face = here, face
    Carried.keep(carry_ref, 0, before, change, low_face)

    ghost_end = arrived(along + 1)
    before = Cells(
        [both(lambda a, b: 0.5 * a + 0.5 * b, a, b) for a, b in zip(ghost_now, ghost_end)]
    )
    low_face, change = None, None
    total_sums = {}
    for index in range(along - 1):
        here = Cells(halves[index])
        face = x_face(before, here)
        if index == 0:
            faces.append(face)
        else:
            state = step_state(before.state, change, face, low_face)
            layer = jnp.where(at_high, along - index, index - 1)
            put_layer(stage_ref, along + 1 + index, new_ref, layer, state, turn)
            for f in range(fields):
                key = (index - 1) // 2, f
                pooled = state[f][0] + state[f][1]
                total_sums[key] = total_sums[key] + pooled if key in total_sums else pooled
        change = side_change(here)
        before, low_face = here, face
    Carried.keep(carry_ref, 1, before, change, low_face)
    keys = sorted(total_sums)
    blocks = [0.125 * total_sums[key] for key in keys]
    for f in range(fields):
        both_steps = [faces[0][f][parity] + faces[1][f][parity] for parity in (0, 1)]
        blocks.append((-0.5 * time_step / 8) * (both_steps[0] + both_steps[1]))
    records = pool_z(jnp.concatenate(blocks, axis=0), face_ref.shape[2])
    for index, (plane, f) in enumerate([*keys, *((None, f) for f in range(fields))]):
        record = records[index * half_across:(index + 1) * half_across]
        record = turn * record if f == 1 else record
        if plane is None:
            face_ref[f] = record
        else:
            sum_ref[plane, f] = record

    for copy in small:
        copy.wait()
    total = owner_vmem.shape[1]
    count_average = (along // 2) * half_across
    selections = one_hot_slots(owner_vmem[...], groups, capacity)
    record_ids = lax.broadcasted_iota(jnp.int32, (1, total), 1)
    codes = (column_vmem[...] + 1).astype(jnp.float32)
    codes = jnp.where(record_ids < count_average, codes, -codes)
    for slot in range(capacity):
        rows = slice(slot * groups, (slot + 1) * groups)
        ids = record_ids.astype(jnp.float32)
        record = jnp.sum(selections[slot] * ids, axis=1, keepdims=True)
        select_ref[rows] = jnp.broadcast_to(record, (groups, code_ref.shape[1])).astype(jnp.int32)
        code = jnp.sum(selections[slot] * codes, axis=1, keepdims=True)
        code_ref[rows] = jnp.broadcast_to(code, (groups, code_ref.shape[1]))


def late_kernel(
    groups, capacity, rows, carry_ref, other_ref, face_ref, sum_ref, select_ref, code_ref,
    early_ref, new_ref, out_ref, stage_ref,
):
    del early_ref
    fields, along, across, depth = other_ref.shape
    half_across = across // 2
    lanes = stage_ref.shape[-1]
    pieces = depth // lanes
    at_high = lax.axis_index("box") == 1
    turn = jnp.where(at_high, -1.0, 1.0)

    def place(index):
        return jnp.where(at_high, along - 1 - index, index)

    def received(index):
        for f in range(fields):
            plane = other_ref[f, place(index)]
            for piece in range(pieces):
                stage_ref[index, f, piece] = plane[:, piece * lanes:(piece + 1) * lanes]
        planes = [split_z(stage_ref, index, f, half_across) for f in range(fields)]
        planes[1] = tuple(turn * values for values in planes[1])
        return planes

    near = Cells(received(0))
    end = Carried(carry_ref, 0, fields)
    end_face = x_face(end, near)
    end_half = end.finished(end_face)
    near_half = step_state(
        near.state, side_change(near), x_face(near, Cells(received(1))), end_face
    )
    inner = Carried(carry_ref, 1, fields)
    last = Cells(end_half)
    inner_face = x_face(inner, last)
    inner_new = inner.finished(inner_face)
    last_new = step_state(
        last.state, side_change(last), x_face(last, Cells(near_half)), inner_face
    )
    put_layer(stage_ref, 2, new_ref, place(along - 2), inner_new, turn)
    put_layer(stage_ref, 3, new_ref, place(along - 1), last_new, turn)

    planes = along // 2
    records = []
    for f in range(fields):
        scale = turn if f == 1 else 1.0
        last_sum = (inner_new[f][0] + inner_new[f][1]) + (last_new[f][0] + last_new[f][1])
        sums = [sum_ref[plane, f] for plane in range(planes - 1)]
        sums.append((0.125 * scale) * pooled_z(last_sum))
        records.append(
            [jnp.where(at_high, sums[planes - 1 - plane], sums[plane]) for plane in range(planes)]
        )
        records[f].append(face_ref[f])
    if half_across == 8 and groups % 8 == 0:
        place_rows(records, select_ref, groups, capacity, rows, out_ref)
    else:
        joined = jnp.concatenate([block for blocks in records for block in blocks], axis=0)
        total = joined.shape[0] // fields
        record_ids = lax.broadcasted_iota(jnp.int32, (capacity * groups, total), 1)
        chosen = jnp.where(select_ref[:, :1] == record_ids, 1.0, 0.0)
        route(joined, chosen, groups, capacity, rows, fields, out_ref)
    for slot in range(capacity):
        out_ref[pl.ds(slot * (fields + 1) + fields, groups, stride=rows), :] = code_ref[
            slot * groups:(slot + 1) * groups
        ]


def pool_z(stacked, coarse_depth):
    depth = stacked.shape[1]
    lane_pair = lax.broadcasted_iota(jnp.int32, (depth, coarse_depth), 0) // 2
    pool = jnp.where(
        lane_pair == lax.broadcasted_iota(jnp.int32, (depth, coarse_depth), 1), 1.0, 0.0
    )
    return split_dot(stacked, pool, True)


def pooled_z(values):
    lanes = 128
    at = lax.broadcasted_iota(jnp.int32, (values.shape[0], lanes), 1)
    even = (at * 2) & (lanes - 1)

    def pairs(start):
        block = values[:, start:start + lanes]
        return jnp.take_along_axis(
            block, even, axis=1, mode="promise_in_bounds"
        ) + jnp.take_along_axis(block, even + 1, axis=1, mode="promise_in_bounds")

    joined = [
        jnp.where(at < lanes // 2, pairs(start), pairs(start + lanes))
        for start in range(0, values.shape[1], 2 * lanes)
    ]
    return joined[0] if len(joined) == 1 else jnp.concatenate(joined, axis=1)


def place_rows(records, select_ref, groups, capacity, rows, out_ref):
    fields = len(records)
    for slot in range(capacity):
        for first in range(0, groups, 8):
            at = slot * groups + first
            chosen = select_ref[at:at + 8]
            row = chosen & 7
            for f in range(fields):
                value = None
                for plane, record in enumerate(records[f]):
                    got = jnp.take_along_axis(record, row, axis=0, mode="promise_in_bounds")
                    value = got if value is None else jnp.where(chosen >= plane * 8, got, value)
                base = first * rows + slot * (fields + 1) + f
                out_ref[pl.ds(base, 8, stride=rows), :] = value


def route(records, selection, groups, capacity, rows, fields, out_ref):
    coarse_depth = out_ref.shape[1]
    total = records.shape[0] // fields
    wide = jnp.concatenate(
        [records[f * total:(f + 1) * total] for f in range(fields)], axis=1
    )
    chosen = split_dot(selection, wide, False)
    for slot in range(capacity):
        for f in range(fields):
            out_ref[pl.ds(slot * (fields + 1) + f, groups, stride=rows), :] = chosen[
                slot * groups:(slot + 1) * groups, f * coarse_depth:(f + 1) * coarse_depth
            ]


def one_hot_slots(owners, groups, capacity):
    total = owners.shape[1]
    hit = owners == lax.broadcasted_iota(jnp.int32, (groups, total), 0)
    hot = jnp.where(hit, 1.0, 0.0)
    earlier = (
        lax.broadcasted_iota(jnp.int32, (total, total), 0)
        < lax.broadcasted_iota(jnp.int32, (total, total), 1)
    )
    rank = jnp.dot(
        hot.astype(jnp.bfloat16),
        jnp.where(earlier, 1.0, 0.0).astype(jnp.bfloat16),
        preferred_element_type=jnp.float32,
    )
    return [jnp.where(hit & (rank == float(slot)), 1.0, 0.0) for slot in range(capacity)]


def patch_kernel(
    box_count, groups, capacity, rows,
    fine_ref, ghost_ref, low_ref, high_ref, owner_ref, column_ref,
    new_ref, out_ref, half_ref, stage_ref,
):
    box_place = lax.axis_index("box")
    at_low = box_place == 0
    at_high = box_place == box_count - 1
    fields, along, across, depth = fine_ref.shape
    half_across = across // 2
    lanes = stage_ref.shape[-1]
    pieces = depth // lanes
    slots = iter(range(stage_ref.shape[0]))

    def parted(planes):
        slot = next(slots)
        for f, plane in enumerate(planes):
            for piece in range(pieces):
                stage_ref[slot, f, piece] = plane[:, piece * lanes:(piece + 1) * lanes]
        return [split_z(stage_ref, slot, f, half_across) for f in range(fields)]

    def rows_of(ref, layer):
        return parted([ref[f, layer] for f in range(fields)])

    def ghost_layer(at, time_frac):
        return parted(
            [
                (1.0 - time_frac) * ghost_ref[0, at, f] + time_frac * ghost_ref[1, at, f]
                for f in range(fields)
            ]
        )

    def half_layer(index):
        return [tuple(half_ref[index, f, parity] for parity in (0, 1)) for f in range(fields)]

    def picked(flag, first, second):
        return [both(lambda a, b: jnp.where(flag, a, b), a, b) for a, b in zip(first, second)]

    width = low_ref.shape[1]
    first = [lambda: rows_of(low_ref, width - 2)]
    first += [lambda: picked(at_low, ghost_layer(0, 0.0), rows_of(low_ref, width - 1))]
    first += [functools.partial(rows_of, fine_ref, index) for index in range(along)]
    first += [lambda: picked(at_high, ghost_layer(1, 0.0), rows_of(high_ref, 0))]
    first += [lambda: rows_of(high_ref, 1)]
    second = [lambda: picked(at_low, ghost_layer(0, 0.5), half_layer(0))]
    second += [functools.partial(half_layer, 1 + index) for index in range(along)]
    second += [lambda: picked(at_high, ghost_layer(1, 0.5), half_layer(along + 1))]
    low_at, high_at = (1, 0), (along + 1, along)
    low_faces, high_faces, sums = [], [], {}

    def keep_half(index, state):
        for f in range(fields):
            for parity in (0, 1):
                half_ref[index - 1, f, parity] = state[f][parity]

    def keep_new(index, state):
        put_layer(stage_ref, next(slots), new_ref, index - 1, state, 1.0)
        for f in range(fields):
            pooled = state[f][0] + state[f][1]
            key = (f, (index - 1) // 2)
            sums[key] = sums[key] + pooled if key in sums else pooled

    def face_keeper(step):
        def keep(index, face):
            if index == low_at[step]:
                low_faces.append(face)
            if index == high_at[step]:
                high_faces.append(face)
        return keep

    advance(first, keep_half, face_keeper(0))
    advance(second, keep_new, face_keeper(1))

    planes = along // 2
    blocks = []
    for f in range(fields):
        blocks += [0.125 * sums[f, plane] for plane in range(planes)]
        low = [low_faces[0][f][parity] + low_faces[1][f][parity] for parity in (0, 1)]
        high = [high_faces[0][f][parity] + high_faces[1][f][parity] for parity in (0, 1)]
        face_sum = jnp.where(at_low, low[0] + low[1], -(high[0] + high[1]))
        blocks.append((-0.5 * time_step / 8) * face_sum)
    total = owner_ref.shape[1]
    selections = one_hot_slots(owner_ref[...], groups, capacity)
    route(
        pool_z(jnp.concatenate(blocks, axis=0), out_ref.shape[1]),
        jnp.concatenate(selections, axis=0), groups, capacity, rows, fields, out_ref,
    )
    record_ids = lax.broadcasted_iota(jnp.int32, (1, total), 1)
    codes = (column_ref[...] + 1).astype(jnp.float32)
    face_code = jnp.where(at_low | at_high, -codes, 0.0)
    codes = jnp.where(record_ids < planes * half_across, codes, face_code)
    for slot in range(capacity):
        code = jnp.sum(selections[slot] * codes, axis=1, keepdims=True)
        out_ref[pl.ds(slot * (fields + 1) + fields, groups, stride=rows), :] = jnp.broadcast_to(
            code, (groups, out_ref.shape[1])
        )


def owner_kernel(
    groups, capacity, rows, in_ref, state_ref, term_ref, new_ref,
    coarse_ref, final_ref, out_ref, copy_sems,
):
    write_fine = pltpu.make_async_copy(new_ref, final_ref, copy_sems.at[0])
    write_fine.start()
    fields, total, coarse_depth = state_ref.shape
    codes, values = [], []
    for slot in range(capacity):
        base = slot * (fields + 1)
        code = in_ref[pl.ds(base + fields, groups, stride=rows), :]
        codes.append(code)
        values.append(
            jnp.concatenate(
                [
                    jnp.where(code != 0.0, in_ref[pl.ds(base + f, groups, stride=rows), :], 0.0)
                    for f in range(fields)
                ],
                axis=1,
            )
        )
    codes = jnp.concatenate(codes, axis=0)
    values = jnp.concatenate(values, axis=0)
    count = codes.shape[0]
    across = jnp.transpose(codes)[:total]
    column = (lax.broadcasted_iota(jnp.int32, (total, count), 0) + 1).astype(jnp.float32)
    hot = jnp.where(jnp.abs(across) == column, 1.0, 0.0)
    kind = jnp.where(codes > 0.0, 1.0, jnp.where(codes < 0.0, -1.0, 0.0))
    flag = jnp.dot(
        hot.astype(jnp.bfloat16), kind.astype(jnp.bfloat16), preferred_element_type=jnp.float32
    )
    got = split_dot(hot, values, False)
    for f in range(fields):
        value = got[:, f * coarse_depth:(f + 1) * coarse_depth]
        state = state_ref[f]
        refluxed = state + (value - term_ref[f])
        out_ref[f] = jnp.where(flag > 0.0, value, jnp.where(flag < 0.0, refluxed, state))
    write_coarse = pltpu.make_async_copy(out_ref, coarse_ref, copy_sems.at[1])
    write_coarse.start()
    write_fine.wait()
    write_coarse.wait()


def on_device(fine_state, patch_ghosts, coarse_state, coarse_face_term, dest_grp, dest_column):
    box_count = lax.axis_size("box")
    group_count = lax.axis_size("grp")
    current = fine_state[0]
    fields, cells_along, cells_across, cells_depth = current.shape
    total = dest_grp.shape[-1]
    capacity = (total + group_count - 1) // group_count
    rows = capacity * (fields + 1)
    inner_rows = math.gcd(rows, 8)
    coarse_depth = cells_depth // 2
    owned_state = coarse_state[0, 0].transpose(1, 0, 2)
    owned_term = coarse_face_term[0, 0].transpose(1, 0, 2)
    params = pltpu.CompilerParams(vmem_limit_bytes=vmem_limit)
    vmem = pl.BlockSpec(memory_space=pltpu.VMEM)
    hbm = pl.BlockSpec(memory_space=pltpu.HBM)
    half_across, pieces = cells_across // 2, cells_depth // 128
    outgoing_shape = jax.ShapeDtypeStruct((group_count * rows, coarse_depth), jnp.float32)

    def stage(count):
        return pltpu.VMEM((count, fields, pieces, cells_across, 128), jnp.float32)

    if box_count == 2:
        other = lax.ppermute(current, "box", [(0, 1), (1, 0)])
        copies = (cells_along + 2) * pieces + 4
        shapes = [
            current.shape,
            (2, 3 * fields, 2, half_across, cells_depth),
            (fields, half_across, coarse_depth),
            (cells_along // 2 - 1, fields, half_across, coarse_depth),
            (capacity * group_count, coarse_depth),
            (capacity * group_count, coarse_depth),
            owned_state.shape,
            owned_term.shape,
        ]
        early, carry, face, sums, selection, codes, owned_state, owned_term = pl.pallas_call(
            functools.partial(early_kernel, group_count, capacity),
            out_shape=[
                pltpu.VMEM(shape, jnp.int32 if index == 4 else jnp.float32)
                for index, shape in enumerate(shapes)
            ],
            in_specs=[hbm] * 6,
            out_specs=[vmem] * len(shapes),
            scratch_shapes=[
                stage(2 * cells_along),
                pltpu.VMEM((1, total), jnp.int32),
                pltpu.VMEM((1, total), jnp.int32),
                pltpu.SemaphoreType.DMA((copies,)),
            ],
            compiler_params=params,
            cost_estimate=pl.CostEstimate(
                flops=200 * current.size, bytes_accessed=8 * current.size, transcendentals=0
            ),
            name="early",
        )(*(
            pltpu.with_memory_space_constraint(values, pltpu.HBM)
            for values in (
                fine_state, patch_ghosts, dest_grp[0], dest_column[0], owned_state, owned_term
            )
        ))
        updated, outgoing = pl.pallas_call(
            functools.partial(late_kernel, group_count, capacity, rows),
            out_shape=[
                pltpu.VMEM(current.shape, jnp.float32),
                pltpu.VMEM(outgoing_shape.shape, jnp.float32),
            ],
            in_specs=[vmem] * 7,
            out_specs=[vmem] * 2,
            scratch_shapes=[stage(4)],
            input_output_aliases={6: 0},
            compiler_params=params,
            name="late",
        )(carry, other, face, sums, selection, codes, early)
    else:
        ends = box_count - 1
        low = lax.ppermute(current[:, -2:], "box", [(i, i + 1) for i in range(ends)])
        high = lax.ppermute(current[:, :2], "box", [(i + 1, i) for i in range(ends)])
        updated, outgoing = pl.pallas_call(
            functools.partial(patch_kernel, box_count, group_count, capacity, rows),
            out_shape=[jax.ShapeDtypeStruct(current.shape, jnp.float32), outgoing_shape],
            in_specs=[vmem] * 6,
            out_specs=[vmem] * 2,
            scratch_shapes=[
                pltpu.VMEM((cells_along + 2, fields, 2, half_across, cells_depth), jnp.float32),
                stage(2 * cells_along + 8),
            ],
            compiler_params=params,
            name="patch",
        )(current, patch_ghosts[0], low, high, dest_grp[0], dest_column[0])
    incoming = lax.all_to_all(
        outgoing.reshape(group_count, rows // inner_rows, inner_rows, coarse_depth),
        "grp", split_axis=0, concat_axis=0, tiled=True,
    ).reshape(group_count * rows, coarse_depth)
    coarse_new, final = pl.pallas_call(
        functools.partial(owner_kernel, group_count, capacity, rows),
        out_shape=[
            jax.ShapeDtypeStruct((fields, total, coarse_depth), jnp.float32),
            jax.ShapeDtypeStruct(current.shape, jnp.float32),
        ],
        in_specs=[vmem] * 4,
        out_specs=[hbm, hbm],
        scratch_shapes=[
            pltpu.VMEM((fields, total, coarse_depth), jnp.float32),
            pltpu.SemaphoreType.DMA((2,)),
        ],
        compiler_params=params,
        name="owner",
    )(
        incoming,
        pltpu.with_memory_space_constraint(owned_state, pltpu.VMEM),
        pltpu.with_memory_space_constraint(owned_term, pltpu.VMEM),
        pltpu.with_memory_space_constraint(updated, pltpu.VMEM),
    )
    return (final[None], coarse_new.transpose(1, 0, 2)[None, None])


def solution(mesh):
    in_specs = (
        P("grp", None, "box", None, None),
        P("grp", None, None, None, None, None),
        P("grp", "box", None, None, None),
        P("grp", "box", None, None, None),
        P("grp", "box", None),
        P("grp", "box", None),
    )
    out_specs = (P("grp", None, "box", None, None), P("grp", "box", None, None, None))
    return jax.shard_map(
        on_device, mesh=mesh, in_specs=in_specs, out_specs=out_specs, check_vma=False
    )
```

```python
import functools
import math

import jax
import jax.numpy as jnp
from jax import lax
from jax.experimental import pallas as pl
from jax.experimental.pallas import tpu as pltpu
from jax.sharding import PartitionSpec as P

gamma_ratio = 1.4
time_step = 0.06
vmem_limit = 8 * 1024 * 1024


def split_dot(lhs, rhs, split_lhs, dims=(((1,), (0,)), ((), ()))):
    data = lhs if split_lhs else rhs
    exact = (rhs if split_lhs else lhs).astype(jnp.bfloat16)
    total = None
    for _ in range(3):
        term = data.astype(jnp.bfloat16)
        data = data - term.astype(jnp.float32)
        pair = (term, exact) if split_lhs else (exact, term)
        part = lax.dot_general(*pair, dims, preferred_element_type=jnp.float32)
        total = part if total is None else total + part
    return total


def next_z(values):
    return pltpu.roll(values, values.shape[-1] - 1, 1)


def last_z(values):
    return pltpu.roll(values, 1, 1)


def next_y(pair):
    even, odd = pair
    return (odd, pltpu.roll(even, even.shape[0] - 1, 0))


def last_y(pair):
    even, odd = pair
    return (pltpu.roll(odd, 1, 0), even)


def both(function, *pairs):
    return tuple(function(*halves) for halves in zip(*pairs))


class Cells:

    def __init__(self, state):
        density, mom = state[0], state[1:4]
        inverse = both(lambda d: 1.0 / d, density)
        velocity = [both(lambda m, r: m * r, m, inverse) for m in mom]
        square = {}
        for i in range(3):
            for j in range(i, 3):
                square[i, j] = both(lambda m, v: m * v, mom[i], velocity[j])
        pressure = both(
            lambda e, a, b, c: (gamma_ratio - 1.0) * (e - 0.5 * (a + b + c)),
            state[4], square[0, 0], square[1, 1], square[2, 2],
        )
        square_sound = both(lambda p, r: gamma_ratio * p * r, pressure, inverse)
        sound = both(lambda q: q * lax.rsqrt(q), square_sound)
        enthalpy = both(jnp.add, state[4], pressure)
        self.state = state
        self.flux = []
        self.speed = []
        for normal in range(3):
            pieces = [mom[normal]]
            for member in range(3):
                term = square[min(member, normal), max(member, normal)]
                pieces.append(both(jnp.add, term, pressure) if member == normal else term)
            pieces.append(both(jnp.multiply, enthalpy, velocity[normal]))
            self.flux.append(pieces)
            self.speed.append(both(lambda v, c: jnp.abs(v) + c, velocity[normal], sound))


def doubled_face(left_state, right_state, left_flux, right_flux, left_speed, right_speed):
    biggest = both(jnp.maximum, left_speed, right_speed)
    return [
        both(lambda a, b, f, g, s: (f + g) - s * (b - a), ls, rs, lf, rf, biggest)
        for ls, rs, lf, rf in zip(left_state, right_state, left_flux, right_flux)
    ]


def x_face(left, right):
    return doubled_face(
        left.state, right.state, left.flux[0], right.flux[0], left.speed[0], right.speed[0]
    )


def side_change(cells):
    change = [None] * len(cells.state)
    for normal in (1, 2):
        if normal == 1:
            ahead, behind = next_y, last_y
        else:
            ahead = functools.partial(both, next_z)
            behind = functools.partial(both, last_z)
        faces = doubled_face(
            cells.state, [ahead(s) for s in cells.state],
            cells.flux[normal], [ahead(f) for f in cells.flux[normal]],
            cells.speed[normal], ahead(cells.speed[normal]),
        )
        for index, face in enumerate(faces):
            part = both(jnp.subtract, face, behind(face))
            change[index] = part if change[index] is None else both(jnp.add, change[index], part)
    return change


def advance(layers, on_update, on_face):
    before, low_face, change = Cells(layers[0]()), None, None
    for index in range(1, len(layers)):
        here = Cells(layers[index]())
        face = x_face(before, here)
        on_face(index - 1, face)
        if index >= 2:
            half = 0.5 * time_step
            on_update(
                index - 1,
                [
                    both(lambda u, c, h, l: u - half * (c + (h - l)), u, c, h, l)
                    for u, c, h, l in zip(before.state, change, face, low_face)
                ],
            )
        if index < len(layers) - 1:
            change = side_change(here)
        before, low_face = here, face


def step_state(state, change, high_face, low_face):
    half = 0.5 * time_step
    return [
        both(lambda u, c, h, l: u - half * (c + (h - l)), u, c, h, l)
        for u, c, h, l in zip(state, change, high_face, low_face)
    ]


def split_z(ref, slot, field, half_across):
    return tuple(
        jnp.concatenate(
            [
                ref[slot, field, piece, pl.ds(parity, half_across, stride=2), :]
                for piece in range(ref.shape[2])
            ],
            axis=1,
        )
        for parity in (0, 1)
    )


def put_layer(stage_ref, slot, new_ref, layer, state, turn):
    fields, pieces, _, lanes = stage_ref.shape[1:]
    half_across = state[0][0].shape[0]
    for f in range(fields):
        for piece in range(pieces):
            part = slice(piece * lanes, (piece + 1) * lanes)
            for parity in (0, 1):
                values = state[f][parity][:, part]
                stage_ref[slot, f, piece, pl.ds(parity, half_across, stride=2), :] = (
                    turn * values if f == 1 else values
                )
            new_ref[f, layer, :, part] = stage_ref[slot, f, piece]


class Carried:

    def __init__(self, ref, slot, fields):
        def pair(index):
            return tuple(ref[slot, index, parity] for parity in (0, 1))

        self.state = [pair(f) for f in range(fields)]
        self.flux = [[self.state[1]] + [pair(fields + f) for f in range(1, fields)]]
        self.speed = [pair(fields)]
        self.partial = [pair(2 * fields + f) for f in range(fields)]

    @staticmethod
    def keep(ref, slot, cells, change, low_face):
        half = 0.5 * time_step
        fields = len(cells.state)
        for f in range(fields):
            for parity in (0, 1):
                ref[slot, f, parity] = cells.state[f][parity]
                ref[slot, 2 * fields + f, parity] = cells.state[f][parity] - half * (
                    change[f][parity] - low_face[f][parity]
                )
                ref[slot, fields + f, parity] = (
                    cells.flux[0][f][parity] if f > 0 else cells.speed[0][parity]
                )

    def finished(self, high_face):
        half = 0.5 * time_step
        return [both(lambda p, h: p - half * h, p, h) for p, h in zip(self.partial, high_face)]


def early_kernel(
    groups, capacity, fine_ref, ghost_ref, owner_ref, column_ref, state_ref, term_ref,
    new_ref, carry_ref, face_ref, sum_ref, select_ref, code_ref, state_vmem, term_vmem,
    stage_ref, owner_vmem, column_vmem, copy_sems,
):
    _, fields, along, across, depth = fine_ref.shape
    half_across = across // 2
    lanes = stage_ref.shape[-1]
    pieces = depth // lanes
    at_high = lax.axis_index("box") == 1
    side = jnp.where(at_high, 1, 0)
    turn = jnp.where(at_high, -1.0, 1.0)

    copies = {}

    def fetch(slot, source):
        for piece in range(pieces):
            copies[slot, piece] = pltpu.make_async_copy(
                source(slice(piece * lanes, (piece + 1) * lanes)),
                stage_ref.at[slot, :, piece],
                copy_sems.at[slot * pieces + piece],
            )
            copies[slot, piece].start()

    ghost_slots = (0, along + 1)
    fetch(0, lambda part: ghost_ref.at[0, 0, side, :, :, part])
    for index in range(along):
        layer = jnp.where(at_high, along - 1 - index, index)
        fetch(1 + index, lambda part, layer=layer: fine_ref.at[0, :, layer, :, part])
    fetch(along + 1, lambda part: ghost_ref.at[0, 1, side, :, :, part])
    pairs = (
        (owner_ref, owner_vmem), (column_ref, column_vmem),
        (state_ref, state_vmem), (term_ref, term_vmem),
    )
    small = [
        pltpu.make_async_copy(source, target, copy_sems.at[(along + 2) * pieces + index])
        for index, (source, target) in enumerate(pairs)
    ]
    for copy in small:
        copy.start()

    def arrived(slot):
        if slot in (0, 3):
            for (at, _), copy in copies.items():
                if (at < 3) == (slot == 0):
                    copy.wait()
        planes = [split_z(stage_ref, slot, f, half_across) for f in range(fields)]
        planes[1] = tuple(turn * values for values in planes[1])
        return planes

    ghost_now = arrived(0)
    before, low_face, change = Cells(ghost_now), None, None
    faces = []
    halves = []
    for index in range(along):
        here = Cells(arrived(1 + index))
        face = x_face(before, here)
        if index == 0:
            faces.append(face)
        else:
            halves.append(step_state(before.state, change, face, low_face))
        change = side_change(here)
        before, low_face = here, face
    Carried.keep(carry_ref, 0, before, change, low_face)

    ghost_end = arrived(along + 1)
    before = Cells(
        [both(lambda a, b: 0.5 * a + 0.5 * b, a, b) for a, b in zip(ghost_now, ghost_end)]
    )
    low_face, change = None, None
    total_sums = {}
    for index in range(along - 1):
        here = Cells(halves[index])
        face = x_face(before, here)
        if index == 0:
            faces.append(face)
        else:
            state = step_state(before.state, change, face, low_face)
            layer = jnp.where(at_high, along - index, index - 1)
            put_layer(stage_ref, along + 1 + index, new_ref, layer, state, turn)
            for f in range(fields):
                key = (index - 1) // 2, f
                pooled = state[f][0] + state[f][1]
                total_sums[key] = total_sums[key] + pooled if key in total_sums else pooled
        change = side_change(here)
        before, low_face = here, face
    Carried.keep(carry_ref, 1, before, change, low_face)
    keys = sorted(total_sums)
    blocks = [0.125 * total_sums[key] for key in keys]
    for f in range(fields):
        both_steps = [faces[0][f][parity] + faces[1][f][parity] for parity in (0, 1)]
        blocks.append((-0.5 * time_step / 8) * (both_steps[0] + both_steps[1]))
    records = pool_z(jnp.concatenate(blocks, axis=0), face_ref.shape[2])
    for index, (plane, f) in enumerate([*keys, *((None, f) for f in range(fields))]):
        record = records[index * half_across:(index + 1) * half_across]
        record = turn * record if f == 1 else record
        if plane is None:
            face_ref[f] = record
        else:
            sum_ref[plane, f] = record

    for copy in small:
        copy.wait()
    total = owner_vmem.shape[1]
    count_average = (along // 2) * half_across
    selections = one_hot_slots(owner_vmem[...], groups, capacity)
    record_ids = lax.broadcasted_iota(jnp.int32, (1, total), 1)
    codes = (column_vmem[...] + 1).astype(jnp.float32)
    codes = jnp.where(record_ids < count_average, codes, -codes)
    for slot in range(capacity):
        rows = slice(slot * groups, (slot + 1) * groups)
        ids = record_ids.astype(jnp.float32)
        record = jnp.sum(selections[slot] * ids, axis=1, keepdims=True)
        select_ref[rows] = jnp.broadcast_to(record, (groups, code_ref.shape[1])).astype(jnp.int32)
        code = jnp.sum(selections[slot] * codes, axis=1, keepdims=True)
        code_ref[rows] = jnp.broadcast_to(code, (groups, code_ref.shape[1]))


def late_kernel(
    groups, capacity, rows, carry_ref, other_ref, face_ref, sum_ref, select_ref, code_ref,
    early_ref, new_ref, out_ref, stage_ref,
):
    del early_ref
    fields, along, across, depth = other_ref.shape
    half_across = across // 2
    lanes = stage_ref.shape[-1]
    pieces = depth // lanes
    at_high = lax.axis_index("box") == 1
    turn = jnp.where(at_high, -1.0, 1.0)

    def place(index):
        return jnp.where(at_high, along - 1 - index, index)

    def received(index):
        for f in range(fields):
            plane = other_ref[f, place(index)]
            for piece in range(pieces):
                stage_ref[index, f, piece] = plane[:, piece * lanes:(piece + 1) * lanes]
        planes = [split_z(stage_ref, index, f, half_across) for f in range(fields)]
        planes[1] = tuple(turn * values for values in planes[1])
        return planes

    near = Cells(received(0))
    end = Carried(carry_ref, 0, fields)
    end_face = x_face(end, near)
    end_half = end.finished(end_face)
    near_half = step_state(
        near.state, side_change(near), x_face(near, Cells(received(1))), end_face
    )
    inner = Carried(carry_ref, 1, fields)
    last = Cells(end_half)
    inner_face = x_face(inner, last)
    inner_new = inner.finished(inner_face)
    last_new = step_state(
        last.state, side_change(last), x_face(last, Cells(near_half)), inner_face
    )
    put_layer(stage_ref, 2, new_ref, place(along - 2), inner_new, turn)
    put_layer(stage_ref, 3, new_ref, place(along - 1), last_new, turn)

    planes = along // 2
    records = []
    for f in range(fields):
        scale = turn if f == 1 else 1.0
        last_sum = (inner_new[f][0] + inner_new[f][1]) + (last_new[f][0] + last_new[f][1])
        sums = [sum_ref[plane, f] for plane in range(planes - 1)]
        sums.append((0.125 * scale) * pooled_z(last_sum))
        records.append(
            [jnp.where(at_high, sums[planes - 1 - plane], sums[plane]) for plane in range(planes)]
        )
        records[f].append(face_ref[f])
    if half_across == 8 and groups % 8 == 0:
        place_rows(records, select_ref, groups, capacity, rows, out_ref)
    else:
        joined = jnp.concatenate([block for blocks in records for block in blocks], axis=0)
        total = joined.shape[0] // fields
        record_ids = lax.broadcasted_iota(jnp.int32, (capacity * groups, total), 1)
        chosen = jnp.where(select_ref[:, :1] == record_ids, 1.0, 0.0)
        route(joined, chosen, groups, capacity, rows, fields, out_ref)
    for slot in range(capacity):
        out_ref[pl.ds(slot * (fields + 1) + fields, groups, stride=rows), :] = code_ref[
            slot * groups:(slot + 1) * groups
        ]


def pool_z(stacked, coarse_depth):
    depth = stacked.shape[1]
    lane_pair = lax.broadcasted_iota(jnp.int32, (depth, coarse_depth), 0) // 2
    pool = jnp.where(
        lane_pair == lax.broadcasted_iota(jnp.int32, (depth, coarse_depth), 1), 1.0, 0.0
    )
    return split_dot(stacked, pool, True)


def pooled_z(values):
    lanes = 128
    at = lax.broadcasted_iota(jnp.int32, (values.shape[0], lanes), 1)
    even = (at * 2) & (lanes - 1)

    def pairs(start):
        block = values[:, start:start + lanes]
        return jnp.take_along_axis(
            block, even, axis=1, mode="promise_in_bounds"
        ) + jnp.take_along_axis(block, even + 1, axis=1, mode="promise_in_bounds")

    joined = [
        jnp.where(at < lanes // 2, pairs(start), pairs(start + lanes))
        for start in range(0, values.shape[1], 2 * lanes)
    ]
    return joined[0] if len(joined) == 1 else jnp.concatenate(joined, axis=1)


def place_rows(records, select_ref, groups, capacity, rows, out_ref):
    fields = len(records)
    for slot in range(capacity):
        for first in range(0, groups, 8):
            at = slot * groups + first
            chosen = select_ref[at:at + 8]
            row = chosen & 7
            for f in range(fields):
                value = None
                for plane, record in enumerate(records[f]):
                    got = jnp.take_along_axis(record, row, axis=0, mode="promise_in_bounds")
                    value = got if value is None else jnp.where(chosen >= plane * 8, got, value)
                base = first * rows + slot * (fields + 1) + f
                out_ref[pl.ds(base, 8, stride=rows), :] = value


def route(records, selection, groups, capacity, rows, fields, out_ref):
    coarse_depth = out_ref.shape[1]
    total = records.shape[0] // fields
    wide = jnp.concatenate(
        [records[f * total:(f + 1) * total] for f in range(fields)], axis=1
    )
    chosen = split_dot(selection, wide, False)
    for slot in range(capacity):
        for f in range(fields):
            out_ref[pl.ds(slot * (fields + 1) + f, groups, stride=rows), :] = chosen[
                slot * groups:(slot + 1) * groups, f * coarse_depth:(f + 1) * coarse_depth
            ]


def one_hot_slots(owners, groups, capacity):
    total = owners.shape[1]
    hit = owners == lax.broadcasted_iota(jnp.int32, (groups, total), 0)
    hot = jnp.where(hit, 1.0, 0.0)
    earlier = (
        lax.broadcasted_iota(jnp.int32, (total, total), 0)
        < lax.broadcasted_iota(jnp.int32, (total, total), 1)
    )
    rank = jnp.dot(
        hot.astype(jnp.bfloat16),
        jnp.where(earlier, 1.0, 0.0).astype(jnp.bfloat16),
        preferred_element_type=jnp.float32,
    )
    return [jnp.where(hit & (rank == float(slot)), 1.0, 0.0) for slot in range(capacity)]


def patch_kernel(
    box_count, groups, capacity, rows,
    fine_ref, ghost_ref, low_ref, high_ref, owner_ref, column_ref,
    new_ref, out_ref, half_ref, stage_ref,
):
    box_place = lax.axis_index("box")
    at_low = box_place == 0
    at_high = box_place == box_count - 1
    fields, along, across, depth = fine_ref.shape
    half_across = across // 2
    lanes = stage_ref.shape[-1]
    pieces = depth // lanes
    slots = iter(range(stage_ref.shape[0]))

    def parted(planes):
        slot = next(slots)
        for f, plane in enumerate(planes):
            for piece in range(pieces):
                stage_ref[slot, f, piece] = plane[:, piece * lanes:(piece + 1) * lanes]
        return [split_z(stage_ref, slot, f, half_across) for f in range(fields)]

    def rows_of(ref, layer):
        return parted([ref[f, layer] for f in range(fields)])

    def ghost_layer(at, time_frac):
        return parted(
            [
                (1.0 - time_frac) * ghost_ref[0, at, f] + time_frac * ghost_ref[1, at, f]
                for f in range(fields)
            ]
        )

    def half_layer(index):
        return [tuple(half_ref[index, f, parity] for parity in (0, 1)) for f in range(fields)]

    def picked(flag, first, second):
        return [both(lambda a, b: jnp.where(flag, a, b), a, b) for a, b in zip(first, second)]

    width = low_ref.shape[1]
    first = [lambda: rows_of(low_ref, width - 2)]
    first += [lambda: picked(at_low, ghost_layer(0, 0.0), rows_of(low_ref, width - 1))]
    first += [functools.partial(rows_of, fine_ref, index) for index in range(along)]
    first += [lambda: picked(at_high, ghost_layer(1, 0.0), rows_of(high_ref, 0))]
    first += [lambda: rows_of(high_ref, 1)]
    second = [lambda: picked(at_low, ghost_layer(0, 0.5), half_layer(0))]
    second += [functools.partial(half_layer, 1 + index) for index in range(along)]
    second += [lambda: picked(at_high, ghost_layer(1, 0.5), half_layer(along + 1))]
    low_at, high_at = (1, 0), (along + 1, along)
    low_faces, high_faces, sums = [], [], {}

    def keep_half(index, state):
        for f in range(fields):
            for parity in (0, 1):
                half_ref[index - 1, f, parity] = state[f][parity]

    def keep_new(index, state):
        put_layer(stage_ref, next(slots), new_ref, index - 1, state, 1.0)
        for f in range(fields):
            pooled = state[f][0] + state[f][1]
            key = (f, (index - 1) // 2)
            sums[key] = sums[key] + pooled if key in sums else pooled

    def face_keeper(step):
        def keep(index, face):
            if index == low_at[step]:
                low_faces.append(face)
            if index == high_at[step]:
                high_faces.append(face)
        return keep

    advance(first, keep_half, face_keeper(0))
    advance(second, keep_new, face_keeper(1))

    planes = along // 2
    blocks = []
    for f in range(fields):
        blocks += [0.125 * sums[f, plane] for plane in range(planes)]
        low = [low_faces[0][f][parity] + low_faces[1][f][parity] for parity in (0, 1)]
        high = [high_faces[0][f][parity] + high_faces[1][f][parity] for parity in (0, 1)]
        face_sum = jnp.where(at_low, low[0] + low[1], -(high[0] + high[1]))
        blocks.append((-0.5 * time_step / 8) * face_sum)
    total = owner_ref.shape[1]
    selections = one_hot_slots(owner_ref[...], groups, capacity)
    route(
        pool_z(jnp.concatenate(blocks, axis=0), out_ref.shape[1]),
        jnp.concatenate(selections, axis=0), groups, capacity, rows, fields, out_ref,
    )
    record_ids = lax.broadcasted_iota(jnp.int32, (1, total), 1)
    codes = (column_ref[...] + 1).astype(jnp.float32)
    face_code = jnp.where(at_low | at_high, -codes, 0.0)
    codes = jnp.where(record_ids < planes * half_across, codes, face_code)
    for slot in range(capacity):
        code = jnp.sum(selections[slot] * codes, axis=1, keepdims=True)
        out_ref[pl.ds(slot * (fields + 1) + fields, groups, stride=rows), :] = jnp.broadcast_to(
            code, (groups, out_ref.shape[1])
        )


def owner_kernel(
    groups, capacity, rows, in_ref, state_ref, term_ref, new_ref,
    coarse_ref, final_ref, out_ref, copy_sems,
):
    write_fine = pltpu.make_async_copy(new_ref, final_ref, copy_sems.at[0])
    write_fine.start()
    fields, total, coarse_depth = state_ref.shape
    codes = jnp.concatenate(
        [
            in_ref[pl.ds(slot * (fields + 1) + fields, groups, stride=rows), :]
            for slot in range(capacity)
        ],
        axis=0,
    )
    count = codes.shape[0]
    across = jnp.transpose(codes)[:total]
    column = (lax.broadcasted_iota(jnp.int32, (total, count), 0) + 1).astype(jnp.float32)
    hit = jnp.abs(across) == column
    place = lax.broadcasted_iota(jnp.int32, (total, count), 1).astype(jnp.float32)
    source = jnp.sum(jnp.where(hit, place, 0.0), axis=1, keepdims=True)
    kind = jnp.sum(jnp.where(hit, across, 0.0), axis=1, keepdims=True)
    source = jnp.broadcast_to(source, (total, coarse_depth)).astype(jnp.int32)
    kind = jnp.broadcast_to(kind, (total, coarse_depth))
    for first in range(0, total, 8):
        part = slice(first, first + 8)
        chosen, sign = source[part], kind[part]
        row = chosen & 7
        for f in range(fields):
            value = None
            for at in range(0, count, 8):
                slot, group = at // groups, at % groups
                base = group * rows + slot * (fields + 1) + f
                got = jnp.take_along_axis(
                    in_ref[pl.ds(base, 8, stride=rows), :], row,
                    axis=0, mode="promise_in_bounds",
                )
                value = got if value is None else jnp.where(chosen >= at, got, value)
            state = state_ref[f, part]
            refluxed = state + (value - term_ref[f, part])
            out_ref[f, part] = jnp.where(
                sign > 0.0, value, jnp.where(sign < 0.0, refluxed, state)
            )
    write_coarse = pltpu.make_async_copy(out_ref, coarse_ref, copy_sems.at[1])
    write_coarse.start()
    write_fine.wait()
    write_coarse.wait()


def on_device(fine_state, patch_ghosts, coarse_state, coarse_face_term, dest_grp, dest_column):
    box_count = lax.axis_size("box")
    group_count = lax.axis_size("grp")
    current = fine_state[0]
    fields, cells_along, cells_across, cells_depth = current.shape
    total = dest_grp.shape[-1]
    capacity = (total + group_count - 1) // group_count
    rows = capacity * (fields + 1)
    inner_rows = math.gcd(rows, 8)
    coarse_depth = cells_depth // 2
    owned_state = coarse_state[0, 0].transpose(1, 0, 2)
    owned_term = coarse_face_term[0, 0].transpose(1, 0, 2)
    params = pltpu.CompilerParams(vmem_limit_bytes=vmem_limit)
    vmem = pl.BlockSpec(memory_space=pltpu.VMEM)
    hbm = pl.BlockSpec(memory_space=pltpu.HBM)
    half_across, pieces = cells_across // 2, cells_depth // 128
    outgoing_shape = jax.ShapeDtypeStruct((group_count * rows, coarse_depth), jnp.float32)

    def stage(count):
        return pltpu.VMEM((count, fields, pieces, cells_across, 128), jnp.float32)

    if box_count == 2:
        other = lax.ppermute(current, "box", [(0, 1), (1, 0)])
        copies = (cells_along + 2) * pieces + 4
        shapes = [
            current.shape,
            (2, 3 * fields, 2, half_across, cells_depth),
            (fields, half_across, coarse_depth),
            (cells_along // 2 - 1, fields, half_across, coarse_depth),
            (capacity * group_count, coarse_depth),
            (capacity * group_count, coarse_depth),
            owned_state.shape,
            owned_term.shape,
        ]
        early, carry, face, sums, selection, codes, owned_state, owned_term = pl.pallas_call(
            functools.partial(early_kernel, group_count, capacity),
            out_shape=[
                pltpu.VMEM(shape, jnp.int32 if index == 4 else jnp.float32)
                for index, shape in enumerate(shapes)
            ],
            in_specs=[hbm] * 6,
            out_specs=[vmem] * len(shapes),
            scratch_shapes=[
                stage(2 * cells_along),
                pltpu.VMEM((1, total), jnp.int32),
                pltpu.VMEM((1, total), jnp.int32),
                pltpu.SemaphoreType.DMA((copies,)),
            ],
            compiler_params=params,
            cost_estimate=pl.CostEstimate(
                flops=200 * current.size, bytes_accessed=8 * current.size, transcendentals=0
            ),
            name="early",
        )(*(
            pltpu.with_memory_space_constraint(values, pltpu.HBM)
            for values in (
                fine_state, patch_ghosts, dest_grp[0], dest_column[0], owned_state, owned_term
            )
        ))
        updated, outgoing = pl.pallas_call(
            functools.partial(late_kernel, group_count, capacity, rows),
            out_shape=[
                pltpu.VMEM(current.shape, jnp.float32),
                pltpu.VMEM(outgoing_shape.shape, jnp.float32),
            ],
            in_specs=[vmem] * 7,
            out_specs=[vmem] * 2,
            scratch_shapes=[stage(4)],
            input_output_aliases={6: 0},
            compiler_params=params,
            name="late",
        )(carry, other, face, sums, selection, codes, early)
    else:
        ends = box_count - 1
        low = lax.ppermute(current[:, -2:], "box", [(i, i + 1) for i in range(ends)])
        high = lax.ppermute(current[:, :2], "box", [(i + 1, i) for i in range(ends)])
        updated, outgoing = pl.pallas_call(
            functools.partial(patch_kernel, box_count, group_count, capacity, rows),
            out_shape=[jax.ShapeDtypeStruct(current.shape, jnp.float32), outgoing_shape],
            in_specs=[vmem] * 6,
            out_specs=[vmem] * 2,
            scratch_shapes=[
                pltpu.VMEM((cells_along + 2, fields, 2, half_across, cells_depth), jnp.float32),
                stage(2 * cells_along + 8),
            ],
            compiler_params=params,
            name="patch",
        )(current, patch_ghosts[0], low, high, dest_grp[0], dest_column[0])
    incoming = lax.all_to_all(
        outgoing.reshape(group_count, rows // inner_rows, inner_rows, coarse_depth),
        "grp", split_axis=0, concat_axis=0, tiled=True,
    ).reshape(group_count * rows, coarse_depth)
    coarse_new, final = pl.pallas_call(
        functools.partial(owner_kernel, group_count, capacity, rows),
        out_shape=[
            jax.ShapeDtypeStruct((fields, total, coarse_depth), jnp.float32),
            jax.ShapeDtypeStruct(current.shape, jnp.float32),
        ],
        in_specs=[vmem] * 4,
        out_specs=[hbm, hbm],
        scratch_shapes=[
            pltpu.VMEM((fields, total, coarse_depth), jnp.float32),
            pltpu.SemaphoreType.DMA((2,)),
        ],
        compiler_params=params,
        name="owner",
    )(
        incoming,
        pltpu.with_memory_space_constraint(owned_state, pltpu.VMEM),
        pltpu.with_memory_space_constraint(owned_term, pltpu.VMEM),
        pltpu.with_memory_space_constraint(updated, pltpu.VMEM),
    )
    return (final[None], coarse_new.transpose(1, 0, 2)[None, None])


def solution(mesh):
    in_specs = (
        P("grp", None, "box", None, None),
        P("grp", None, None, None, None, None),
        P("grp", "box", None, None, None),
        P("grp", "box", None, None, None),
        P("grp", "box", None),
        P("grp", "box", None),
    )
    out_specs = (P("grp", None, "box", None, None), P("grp", "box", None, None, None))
    return jax.shard_map(
        on_device, mesh=mesh, in_specs=in_specs, out_specs=out_specs, check_vma=False
    )
```

```python
import functools
import math

import jax
import jax.numpy as jnp
from jax import lax
from jax.experimental import pallas as pl
from jax.experimental.pallas import tpu as pltpu
from jax.sharding import PartitionSpec as P

gamma_ratio = 1.4
time_step = 0.06
vmem_limit = 8 * 1024 * 1024


def split_dot(lhs, rhs, split_lhs, dims=(((1,), (0,)), ((), ()))):
    data = lhs if split_lhs else rhs
    exact = (rhs if split_lhs else lhs).astype(jnp.bfloat16)
    total = None
    for _ in range(3):
        term = data.astype(jnp.bfloat16)
        data = data - term.astype(jnp.float32)
        pair = (term, exact) if split_lhs else (exact, term)
        part = lax.dot_general(*pair, dims, preferred_element_type=jnp.float32)
        total = part if total is None else total + part
    return total


def next_z(values):
    return pltpu.roll(values, values.shape[-1] - 1, 1)


def last_z(values):
    return pltpu.roll(values, 1, 1)


def next_y(pair):
    even, odd = pair
    return (odd, pltpu.roll(even, even.shape[0] - 1, 0))


def last_y(pair):
    even, odd = pair
    return (pltpu.roll(odd, 1, 0), even)


def both(function, *pairs):
    return tuple(function(*halves) for halves in zip(*pairs))


class Cells:

    def __init__(self, state):
        density, mom = state[0], state[1:4]
        inverse = both(lambda d: 1.0 / d, density)
        velocity = [both(lambda m, r: m * r, m, inverse) for m in mom]
        square = {}
        for i in range(3):
            for j in range(i, 3):
                square[i, j] = both(lambda m, v: m * v, mom[i], velocity[j])
        pressure = both(
            lambda e, a, b, c: (gamma_ratio - 1.0) * (e - 0.5 * (a + b + c)),
            state[4], square[0, 0], square[1, 1], square[2, 2],
        )
        square_sound = both(lambda p, r: gamma_ratio * p * r, pressure, inverse)
        sound = both(lambda q: q * lax.rsqrt(q), square_sound)
        enthalpy = both(jnp.add, state[4], pressure)
        self.state = state
        self.flux = []
        self.speed = []
        for normal in range(3):
            pieces = [mom[normal]]
            for member in range(3):
                term = square[min(member, normal), max(member, normal)]
                pieces.append(both(jnp.add, term, pressure) if member == normal else term)
            pieces.append(both(jnp.multiply, enthalpy, velocity[normal]))
            self.flux.append(pieces)
            self.speed.append(both(lambda v, c: jnp.abs(v) + c, velocity[normal], sound))


def doubled_face(left_state, right_state, left_flux, right_flux, left_speed, right_speed):
    biggest = both(jnp.maximum, left_speed, right_speed)
    return [
        both(lambda a, b, f, g, s: (f + g) - s * (b - a), ls, rs, lf, rf, biggest)
        for ls, rs, lf, rf in zip(left_state, right_state, left_flux, right_flux)
    ]


def x_face(left, right):
    return doubled_face(
        left.state, right.state, left.flux[0], right.flux[0], left.speed[0], right.speed[0]
    )


def side_change(cells):
    change = [None] * len(cells.state)
    for normal in (1, 2):
        if normal == 1:
            ahead, behind = next_y, last_y
        else:
            ahead = functools.partial(both, next_z)
            behind = functools.partial(both, last_z)
        faces = doubled_face(
            cells.state, [ahead(s) for s in cells.state],
            cells.flux[normal], [ahead(f) for f in cells.flux[normal]],
            cells.speed[normal], ahead(cells.speed[normal]),
        )
        for index, face in enumerate(faces):
            part = both(jnp.subtract, face, behind(face))
            change[index] = part if change[index] is None else both(jnp.add, change[index], part)
    return change


def advance(layers, on_update, on_face):
    before, low_face, change = Cells(layers[0]()), None, None
    for index in range(1, len(layers)):
        here = Cells(layers[index]())
        face = x_face(before, here)
        on_face(index - 1, face)
        if index >= 2:
            half = 0.5 * time_step
            on_update(
                index - 1,
                [
                    both(lambda u, c, h, l: u - half * (c + (h - l)), u, c, h, l)
                    for u, c, h, l in zip(before.state, change, face, low_face)
                ],
            )
        if index < len(layers) - 1:
            change = side_change(here)
        before, low_face = here, face


def step_state(state, change, high_face, low_face):
    half = 0.5 * time_step
    return [
        both(lambda u, c, h, l: u - half * (c + (h - l)), u, c, h, l)
        for u, c, h, l in zip(state, change, high_face, low_face)
    ]


def split_z(ref, slot, field, half_across):
    return tuple(
        jnp.concatenate(
            [
                ref[slot, field, piece, pl.ds(parity, half_across, stride=2), :]
                for piece in range(ref.shape[2])
            ],
            axis=1,
        )
        for parity in (0, 1)
    )


def put_layer(stage_ref, slot, new_ref, layer, state, turn):
    fields, pieces, _, lanes = stage_ref.shape[1:]
    half_across = state[0][0].shape[0]
    for f in range(fields):
        for piece in range(pieces):
            part = slice(piece * lanes, (piece + 1) * lanes)
            for parity in (0, 1):
                values = state[f][parity][:, part]
                stage_ref[slot, f, piece, pl.ds(parity, half_across, stride=2), :] = (
                    turn * values if f == 1 else values
                )
            new_ref[f, layer, :, part] = stage_ref[slot, f, piece]


class Carried:

    def __init__(self, ref, slot, fields):
        def pair(index):
            return tuple(ref[slot, index, parity] for parity in (0, 1))

        self.state = [pair(f) for f in range(fields)]
        self.flux = [[self.state[1]] + [pair(fields + f) for f in range(1, fields)]]
        self.speed = [pair(fields)]
        self.partial = [pair(2 * fields + f) for f in range(fields)]

    @staticmethod
    def keep(ref, slot, cells, change, low_face):
        half = 0.5 * time_step
        fields = len(cells.state)
        for f in range(fields):
            for parity in (0, 1):
                ref[slot, f, parity] = cells.state[f][parity]
                ref[slot, 2 * fields + f, parity] = cells.state[f][parity] - half * (
                    change[f][parity] - low_face[f][parity]
                )
                ref[slot, fields + f, parity] = (
                    cells.flux[0][f][parity] if f > 0 else cells.speed[0][parity]
                )

    def finished(self, high_face):
        half = 0.5 * time_step
        return [both(lambda p, h: p - half * h, p, h) for p, h in zip(self.partial, high_face)]


def joined_codes(selections, codes, lanes):
    groups, share = selections[0].shape[0], lanes // len(selections)
    at = lax.broadcasted_iota(jnp.int32, (groups, lanes), 1)
    joined = None
    for slot, selection in enumerate(selections):
        code = jnp.sum(selection * codes, axis=1, keepdims=True)
        code = jnp.broadcast_to(code, (groups, lanes))
        joined = code if joined is None else jnp.where(at >= slot * share, code, joined)
    return joined


def early_kernel(
    groups, capacity, fine_ref, ghost_ref, owner_ref, column_ref, state_ref, term_ref,
    new_ref, carry_ref, face_ref, sum_ref, select_ref, code_ref, state_vmem, term_vmem,
    stage_ref, owner_vmem, column_vmem, copy_sems,
):
    _, fields, along, across, depth = fine_ref.shape
    half_across = across // 2
    lanes = stage_ref.shape[-1]
    pieces = depth // lanes
    at_high = lax.axis_index("box") == 1
    side = jnp.where(at_high, 1, 0)
    turn = jnp.where(at_high, -1.0, 1.0)

    copies = {}

    def fetch(slot, source):
        for piece in range(pieces):
            copies[slot, piece] = pltpu.make_async_copy(
                source(slice(piece * lanes, (piece + 1) * lanes)),
                stage_ref.at[slot, :, piece],
                copy_sems.at[slot * pieces + piece],
            )
            copies[slot, piece].start()

    ghost_slots = (0, along + 1)
    fetch(0, lambda part: ghost_ref.at[0, 0, side, :, :, part])
    for index in range(along):
        layer = jnp.where(at_high, along - 1 - index, index)
        fetch(1 + index, lambda part, layer=layer: fine_ref.at[0, :, layer, :, part])
    fetch(along + 1, lambda part: ghost_ref.at[0, 1, side, :, :, part])
    pairs = (
        (owner_ref, owner_vmem), (column_ref, column_vmem),
        (state_ref, state_vmem), (term_ref, term_vmem),
    )
    small = [
        pltpu.make_async_copy(source, target, copy_sems.at[(along + 2) * pieces + index])
        for index, (source, target) in enumerate(pairs)
    ]
    for copy in small:
        copy.start()

    def arrived(slot):
        if slot in (0, 3):
            for (at, _), copy in copies.items():
                if (at < 3) == (slot == 0):
                    copy.wait()
        planes = [split_z(stage_ref, slot, f, half_across) for f in range(fields)]
        planes[1] = tuple(turn * values for values in planes[1])
        return planes

    ghost_now = arrived(0)
    before, low_face, change = Cells(ghost_now), None, None
    faces = []
    halves = []
    for index in range(along):
        here = Cells(arrived(1 + index))
        face = x_face(before, here)
        if index == 0:
            faces.append(face)
        else:
            halves.append(step_state(before.state, change, face, low_face))
        change = side_change(here)
        before, low_face = here, face
    Carried.keep(carry_ref, 0, before, change, low_face)

    ghost_end = arrived(along + 1)
    before = Cells(
        [both(lambda a, b: 0.5 * a + 0.5 * b, a, b) for a, b in zip(ghost_now, ghost_end)]
    )
    low_face, change = None, None
    total_sums = {}
    for index in range(along - 1):
        here = Cells(halves[index])
        face = x_face(before, here)
        if index == 0:
            faces.append(face)
        else:
            state = step_state(before.state, change, face, low_face)
            layer = jnp.where(at_high, along - index, index - 1)
            put_layer(stage_ref, along + 1 + index, new_ref, layer, state, turn)
            for f in range(fields):
                key = (index - 1) // 2, f
                pooled = state[f][0] + state[f][1]
                total_sums[key] = total_sums[key] + pooled if key in total_sums else pooled
        change = side_change(here)
        before, low_face = here, face
    Carried.keep(carry_ref, 1, before, change, low_face)
    keys = sorted(total_sums)
    blocks = [0.125 * total_sums[key] for key in keys]
    for f in range(fields):
        both_steps = [faces[0][f][parity] + faces[1][f][parity] for parity in (0, 1)]
        blocks.append((-0.5 * time_step / 8) * (both_steps[0] + both_steps[1]))
    records = pool_z(jnp.concatenate(blocks, axis=0), face_ref.shape[2])
    for index, (plane, f) in enumerate([*keys, *((None, f) for f in range(fields))]):
        record = records[index * half_across:(index + 1) * half_across]
        record = turn * record if f == 1 else record
        if plane is None:
            face_ref[f] = record
        else:
            sum_ref[plane, f] = record

    for copy in small:
        copy.wait()
    total = owner_vmem.shape[1]
    count_average = (along // 2) * half_across
    selections = one_hot_slots(owner_vmem[...], groups, capacity)
    record_ids = lax.broadcasted_iota(jnp.int32, (1, total), 1)
    codes = (column_vmem[...] + 1).astype(jnp.float32)
    codes = jnp.where(record_ids < count_average, codes, -codes)
    for slot in range(capacity):
        rows = slice(slot * groups, (slot + 1) * groups)
        ids = record_ids.astype(jnp.float32)
        record = jnp.sum(selections[slot] * ids, axis=1, keepdims=True)
        select_ref[rows] = jnp.broadcast_to(record, (groups, code_ref.shape[1])).astype(jnp.int32)
    code_ref[...] = joined_codes(selections, codes, code_ref.shape[1])


def late_kernel(
    groups, capacity, rows, carry_ref, other_ref, face_ref, sum_ref, select_ref, code_ref,
    early_ref, new_ref, out_ref, stage_ref,
):
    del early_ref
    fields, along, across, depth = other_ref.shape
    half_across = across // 2
    lanes = stage_ref.shape[-1]
    pieces = depth // lanes
    at_high = lax.axis_index("box") == 1
    turn = jnp.where(at_high, -1.0, 1.0)

    def place(index):
        return jnp.where(at_high, along - 1 - index, index)

    def received(index):
        for f in range(fields):
            plane = other_ref[f, place(index)]
            for piece in range(pieces):
                stage_ref[index, f, piece] = plane[:, piece * lanes:(piece + 1) * lanes]
        planes = [split_z(stage_ref, index, f, half_across) for f in range(fields)]
        planes[1] = tuple(turn * values for values in planes[1])
        return planes

    near = Cells(received(0))
    end = Carried(carry_ref, 0, fields)
    end_face = x_face(end, near)
    end_half = end.finished(end_face)
    near_half = step_state(
        near.state, side_change(near), x_face(near, Cells(received(1))), end_face
    )
    inner = Carried(carry_ref, 1, fields)
    last = Cells(end_half)
    inner_face = x_face(inner, last)
    inner_new = inner.finished(inner_face)
    last_new = step_state(
        last.state, side_change(last), x_face(last, Cells(near_half)), inner_face
    )
    put_layer(stage_ref, 2, new_ref, place(along - 2), inner_new, turn)
    put_layer(stage_ref, 3, new_ref, place(along - 1), last_new, turn)

    planes = along // 2
    records = []
    for f in range(fields):
        scale = turn if f == 1 else 1.0
        last_sum = (inner_new[f][0] + inner_new[f][1]) + (last_new[f][0] + last_new[f][1])
        sums = [sum_ref[plane, f] for plane in range(planes - 1)]
        sums.append((0.125 * scale) * pooled_z(last_sum))
        records.append(
            [jnp.where(at_high, sums[planes - 1 - plane], sums[plane]) for plane in range(planes)]
        )
        records[f].append(face_ref[f])
    if half_across == 8 and groups % 8 == 0:
        place_rows(records, select_ref, groups, capacity, rows, out_ref)
    else:
        joined = jnp.concatenate([block for blocks in records for block in blocks], axis=0)
        total = joined.shape[0] // fields
        record_ids = lax.broadcasted_iota(jnp.int32, (capacity * groups, total), 1)
        chosen = jnp.where(select_ref[:, :1] == record_ids, 1.0, 0.0)
        route(joined, chosen, groups, capacity, rows, fields, out_ref)
    out_ref[pl.ds(capacity * fields, groups, stride=rows), :] = code_ref[...]


def pool_z(stacked, coarse_depth):
    depth = stacked.shape[1]
    lane_pair = lax.broadcasted_iota(jnp.int32, (depth, coarse_depth), 0) // 2
    pool = jnp.where(
        lane_pair == lax.broadcasted_iota(jnp.int32, (depth, coarse_depth), 1), 1.0, 0.0
    )
    return split_dot(stacked, pool, True)


def pooled_z(values):
    lanes = 128
    at = lax.broadcasted_iota(jnp.int32, (values.shape[0], lanes), 1)
    even = (at * 2) & (lanes - 1)

    def pairs(start):
        block = values[:, start:start + lanes]
        return jnp.take_along_axis(
            block, even, axis=1, mode="promise_in_bounds"
        ) + jnp.take_along_axis(block, even + 1, axis=1, mode="promise_in_bounds")

    joined = [
        jnp.where(at < lanes // 2, pairs(start), pairs(start + lanes))
        for start in range(0, values.shape[1], 2 * lanes)
    ]
    return joined[0] if len(joined) == 1 else jnp.concatenate(joined, axis=1)


def place_rows(records, select_ref, groups, capacity, rows, out_ref):
    fields = len(records)
    for slot in range(capacity):
        for first in range(0, groups, 8):
            at = slot * groups + first
            chosen = select_ref[at:at + 8]
            row = chosen & 7
            for f in range(fields):
                value = None
                for plane, record in enumerate(records[f]):
                    got = jnp.take_along_axis(record, row, axis=0, mode="promise_in_bounds")
                    value = got if value is None else jnp.where(chosen >= plane * 8, got, value)
                base = first * rows + slot * fields + f
                out_ref[pl.ds(base, 8, stride=rows), :] = value


def route(records, selection, groups, capacity, rows, fields, out_ref):
    coarse_depth = out_ref.shape[1]
    total = records.shape[0] // fields
    wide = jnp.concatenate(
        [records[f * total:(f + 1) * total] for f in range(fields)], axis=1
    )
    chosen = split_dot(selection, wide, False)
    for slot in range(capacity):
        for f in range(fields):
            out_ref[pl.ds(slot * fields + f, groups, stride=rows), :] = chosen[
                slot * groups:(slot + 1) * groups, f * coarse_depth:(f + 1) * coarse_depth
            ]


def one_hot_slots(owners, groups, capacity):
    total = owners.shape[1]
    hit = owners == lax.broadcasted_iota(jnp.int32, (groups, total), 0)
    hot = jnp.where(hit, 1.0, 0.0)
    earlier = (
        lax.broadcasted_iota(jnp.int32, (total, total), 0)
        < lax.broadcasted_iota(jnp.int32, (total, total), 1)
    )
    rank = jnp.dot(
        hot.astype(jnp.bfloat16),
        jnp.where(earlier, 1.0, 0.0).astype(jnp.bfloat16),
        preferred_element_type=jnp.float32,
    )
    return [jnp.where(hit & (rank == float(slot)), 1.0, 0.0) for slot in range(capacity)]


def patch_kernel(
    box_count, groups, capacity, rows,
    fine_ref, ghost_ref, low_ref, high_ref, owner_ref, column_ref,
    new_ref, out_ref, half_ref, stage_ref,
):
    box_place = lax.axis_index("box")
    at_low = box_place == 0
    at_high = box_place == box_count - 1
    fields, along, across, depth = fine_ref.shape
    half_across = across // 2
    lanes = stage_ref.shape[-1]
    pieces = depth // lanes
    slots = iter(range(stage_ref.shape[0]))

    def parted(planes):
        slot = next(slots)
        for f, plane in enumerate(planes):
            for piece in range(pieces):
                stage_ref[slot, f, piece] = plane[:, piece * lanes:(piece + 1) * lanes]
        return [split_z(stage_ref, slot, f, half_across) for f in range(fields)]

    def rows_of(ref, layer):
        return parted([ref[f, layer] for f in range(fields)])

    def ghost_layer(at, time_frac):
        return parted(
            [
                (1.0 - time_frac) * ghost_ref[0, at, f] + time_frac * ghost_ref[1, at, f]
                for f in range(fields)
            ]
        )

    def half_layer(index):
        return [tuple(half_ref[index, f, parity] for parity in (0, 1)) for f in range(fields)]

    def picked(flag, first, second):
        return [both(lambda a, b: jnp.where(flag, a, b), a, b) for a, b in zip(first, second)]

    width = low_ref.shape[1]
    first = [lambda: rows_of(low_ref, width - 2)]
    first += [lambda: picked(at_low, ghost_layer(0, 0.0), rows_of(low_ref, width - 1))]
    first += [functools.partial(rows_of, fine_ref, index) for index in range(along)]
    first += [lambda: picked(at_high, ghost_layer(1, 0.0), rows_of(high_ref, 0))]
    first += [lambda: rows_of(high_ref, 1)]
    second = [lambda: picked(at_low, ghost_layer(0, 0.5), half_layer(0))]
    second += [functools.partial(half_layer, 1 + index) for index in range(along)]
    second += [lambda: picked(at_high, ghost_layer(1, 0.5), half_layer(along + 1))]
    low_at, high_at = (1, 0), (along + 1, along)
    low_faces, high_faces, sums = [], [], {}

    def keep_half(index, state):
        for f in range(fields):
            for parity in (0, 1):
                half_ref[index - 1, f, parity] = state[f][parity]

    def keep_new(index, state):
        put_layer(stage_ref, next(slots), new_ref, index - 1, state, 1.0)
        for f in range(fields):
            pooled = state[f][0] + state[f][1]
            key = (f, (index - 1) // 2)
            sums[key] = sums[key] + pooled if key in sums else pooled

    def face_keeper(step):
        def keep(index, face):
            if index == low_at[step]:
                low_faces.append(face)
            if index == high_at[step]:
                high_faces.append(face)
        return keep

    advance(first, keep_half, face_keeper(0))
    advance(second, keep_new, face_keeper(1))

    planes = along // 2
    blocks = []
    for f in range(fields):
        blocks += [0.125 * sums[f, plane] for plane in range(planes)]
        low = [low_faces[0][f][parity] + low_faces[1][f][parity] for parity in (0, 1)]
        high = [high_faces[0][f][parity] + high_faces[1][f][parity] for parity in (0, 1)]
        face_sum = jnp.where(at_low, low[0] + low[1], -(high[0] + high[1]))
        blocks.append((-0.5 * time_step / 8) * face_sum)
    total = owner_ref.shape[1]
    selections = one_hot_slots(owner_ref[...], groups, capacity)
    route(
        pool_z(jnp.concatenate(blocks, axis=0), out_ref.shape[1]),
        jnp.concatenate(selections, axis=0), groups, capacity, rows, fields, out_ref,
    )
    record_ids = lax.broadcasted_iota(jnp.int32, (1, total), 1)
    codes = (column_ref[...] + 1).astype(jnp.float32)
    face_code = jnp.where(at_low | at_high, -codes, 0.0)
    codes = jnp.where(record_ids < planes * half_across, codes, face_code)
    out_ref[pl.ds(capacity * fields, groups, stride=rows), :] = joined_codes(
        selections, codes, out_ref.shape[1]
    )


def owner_kernel(
    groups, capacity, rows, in_ref, state_ref, term_ref, new_ref,
    coarse_ref, final_ref, out_ref, copy_sems,
):
    write_fine = pltpu.make_async_copy(new_ref, final_ref, copy_sems.at[0])
    write_fine.start()
    fields, total, coarse_depth = state_ref.shape
    count, share = capacity * groups, coarse_depth // capacity
    lanes = jnp.transpose(in_ref[pl.ds(capacity * fields, groups, stride=rows), :])
    column = (lax.broadcasted_iota(jnp.int32, (total, groups), 0) + 1).astype(jnp.float32)
    place = lax.broadcasted_iota(jnp.int32, (total, groups), 1).astype(jnp.float32)
    places = kinds = jnp.zeros((total, groups), jnp.float32)
    for slot in range(capacity):
        across = lanes[slot * share:slot * share + total]
        hit = jnp.abs(across) == column
        places = jnp.where(hit, place + float(slot * groups), places)
        kinds = jnp.where(hit, across, kinds)
    source = jnp.sum(places, axis=1, keepdims=True)
    kind = jnp.sum(kinds, axis=1, keepdims=True)
    source = jnp.broadcast_to(source, (total, coarse_depth)).astype(jnp.int32)
    kind = jnp.broadcast_to(kind, (total, coarse_depth))
    for first in range(0, total, 8):
        part = slice(first, first + 8)
        chosen, sign = source[part], kind[part]
        row = chosen & 7
        for f in range(fields):
            value = None
            for at in range(0, count, 8):
                slot, group = at // groups, at % groups
                base = group * rows + slot * fields + f
                got = jnp.take_along_axis(
                    in_ref[pl.ds(base, 8, stride=rows), :], row,
                    axis=0, mode="promise_in_bounds",
                )
                value = got if value is None else jnp.where(chosen >= at, got, value)
            state = state_ref[f, part]
            refluxed = state + (value - term_ref[f, part])
            out_ref[f, part] = jnp.where(
                sign > 0.0, value, jnp.where(sign < 0.0, refluxed, state)
            )
    write_coarse = pltpu.make_async_copy(out_ref, coarse_ref, copy_sems.at[1])
    write_coarse.start()
    write_fine.wait()
    write_coarse.wait()


def on_device(fine_state, patch_ghosts, coarse_state, coarse_face_term, dest_grp, dest_column):
    box_count = lax.axis_size("box")
    group_count = lax.axis_size("grp")
    current = fine_state[0]
    fields, cells_along, cells_across, cells_depth = current.shape
    total = dest_grp.shape[-1]
    capacity = (total + group_count - 1) // group_count
    rows = capacity * fields + 1
    inner_rows = math.gcd(rows, 8)
    coarse_depth = cells_depth // 2
    owned_state = coarse_state[0, 0].transpose(1, 0, 2)
    owned_term = coarse_face_term[0, 0].transpose(1, 0, 2)
    params = pltpu.CompilerParams(vmem_limit_bytes=vmem_limit)
    vmem = pl.BlockSpec(memory_space=pltpu.VMEM)
    hbm = pl.BlockSpec(memory_space=pltpu.HBM)
    half_across, pieces = cells_across // 2, cells_depth // 128
    outgoing_shape = jax.ShapeDtypeStruct((group_count * rows, coarse_depth), jnp.float32)

    def stage(count):
        return pltpu.VMEM((count, fields, pieces, cells_across, 128), jnp.float32)

    if box_count == 2:
        other = lax.ppermute(current, "box", [(0, 1), (1, 0)])
        copies = (cells_along + 2) * pieces + 4
        shapes = [
            current.shape,
            (2, 3 * fields, 2, half_across, cells_depth),
            (fields, half_across, coarse_depth),
            (cells_along // 2 - 1, fields, half_across, coarse_depth),
            (capacity * group_count, coarse_depth),
            (group_count, coarse_depth),
            owned_state.shape,
            owned_term.shape,
        ]
        early, carry, face, sums, selection, codes, owned_state, owned_term = pl.pallas_call(
            functools.partial(early_kernel, group_count, capacity),
            out_shape=[
                pltpu.VMEM(shape, jnp.int32 if index == 4 else jnp.float32)
                for index, shape in enumerate(shapes)
            ],
            in_specs=[hbm] * 6,
            out_specs=[vmem] * len(shapes),
            scratch_shapes=[
                stage(2 * cells_along),
                pltpu.VMEM((1, total), jnp.int32),
                pltpu.VMEM((1, total), jnp.int32),
                pltpu.SemaphoreType.DMA((copies,)),
            ],
            compiler_params=params,
            cost_estimate=pl.CostEstimate(
                flops=200 * current.size, bytes_accessed=8 * current.size, transcendentals=0
            ),
            name="early",
        )(*(
            pltpu.with_memory_space_constraint(values, pltpu.HBM)
            for values in (
                fine_state, patch_ghosts, dest_grp[0], dest_column[0], owned_state, owned_term
            )
        ))
        updated, outgoing = pl.pallas_call(
            functools.partial(late_kernel, group_count, capacity, rows),
            out_shape=[
                pltpu.VMEM(current.shape, jnp.float32),
                pltpu.VMEM(outgoing_shape.shape, jnp.float32),
            ],
            in_specs=[vmem] * 7,
            out_specs=[vmem] * 2,
            scratch_shapes=[stage(4)],
            input_output_aliases={6: 0},
            compiler_params=params,
            name="late",
        )(carry, other, face, sums, selection, codes, early)
    else:
        ends = box_count - 1
        low = lax.ppermute(current[:, -2:], "box", [(i, i + 1) for i in range(ends)])
        high = lax.ppermute(current[:, :2], "box", [(i + 1, i) for i in range(ends)])
        updated, outgoing = pl.pallas_call(
            functools.partial(patch_kernel, box_count, group_count, capacity, rows),
            out_shape=[jax.ShapeDtypeStruct(current.shape, jnp.float32), outgoing_shape],
            in_specs=[vmem] * 6,
            out_specs=[vmem] * 2,
            scratch_shapes=[
                pltpu.VMEM((cells_along + 2, fields, 2, half_across, cells_depth), jnp.float32),
                stage(2 * cells_along + 8),
            ],
            compiler_params=params,
            name="patch",
        )(current, patch_ghosts[0], low, high, dest_grp[0], dest_column[0])
    incoming = lax.all_to_all(
        outgoing.reshape(group_count, rows // inner_rows, inner_rows, coarse_depth),
        "grp", split_axis=0, concat_axis=0, tiled=True,
    ).reshape(group_count * rows, coarse_depth)
    coarse_new, final = pl.pallas_call(
        functools.partial(owner_kernel, group_count, capacity, rows),
        out_shape=[
            jax.ShapeDtypeStruct((fields, total, coarse_depth), jnp.float32),
            jax.ShapeDtypeStruct(current.shape, jnp.float32),
        ],
        in_specs=[vmem] * 4,
        out_specs=[hbm, hbm],
        scratch_shapes=[
            pltpu.VMEM((fields, total, coarse_depth), jnp.float32),
            pltpu.SemaphoreType.DMA((2,)),
        ],
        compiler_params=params,
        name="owner",
    )(
        incoming,
        pltpu.with_memory_space_constraint(owned_state, pltpu.VMEM),
        pltpu.with_memory_space_constraint(owned_term, pltpu.VMEM),
        pltpu.with_memory_space_constraint(updated, pltpu.VMEM),
    )
    return (final[None], coarse_new.transpose(1, 0, 2)[None, None])


def solution(mesh):
    in_specs = (
        P("grp", None, "box", None, None),
        P("grp", None, None, None, None, None),
        P("grp", "box", None, None, None),
        P("grp", "box", None, None, None),
        P("grp", "box", None),
        P("grp", "box", None),
    )
    out_specs = (P("grp", None, "box", None, None), P("grp", "box", None, None, None))
    return jax.shard_map(
        on_device, mesh=mesh, in_specs=in_specs, out_specs=out_specs, check_vma=False
    )
```
